32 devices in a mesh: dp: 8 (over z, y), mp: 4 (over x, core).
Axes of the slice: x: 2, y: 2, z: 4, core: 2. Of those that a mesh axis runs over, the one named last changes fastest.
Arguments:
- tokens: bfloat16 [16384, 768], P(('dp', 'mp')), may hold values from -6 to 6
- segment_lengths: int32 [32, 8], P('dp'), may hold values from 1 to 192, 512 in all within a row
- gain_one: float32 [768], replicated, may hold values from 0.5 to 1.5
- shift_one: float32 [768], replicated, may hold values from -1.25 to 1.25
- qkv_weight: bfloat16 [3, 768, 768], P(None, None, 'mp'), may hold values from -0.21875 to 0.21875
- qv_bias: float32 [2, 768], P(None, 'mp'), may hold values from -1.75 to 1.75
- out_weight: bfloat16 [768, 768], P('mp'), may hold values from -1.25 to 1.25
- out_bias: float32 [768], replicated, may hold values from -1.25 to 1.25
- gain_two: float32 [768], replicated, may hold values from 0.5 to 1.5
- shift_two: float32 [768], replicated, may hold values from -1.25 to 1.25
- up_weight: bfloat16 [768, 3072], P(None, 'mp'), may hold values from -0.21875 to 0.21875
- up_bias: float32 [3072], P('mp'), may hold values from -1.75 to 1.75
- down_weight: bfloat16 [3072, 768], P('mp'), may hold values from -0.109375 to 0.109375
- down_bias: float32 [768], replicated, may hold values from -1.25 to 1.25
- cotangent: bfloat16 [16384, 768], P(('dp', 'mp')), may hold values from -8 to 8
Outputs:
- layer_output: float32 [16384, 768], P(('dp', 'mp'))
- token_grad: float32 [16384, 768], P(('dp', 'mp'))
- gain_one_grad: float32 [768], replicated
- shift_one_grad: float32 [768], replicated
- qkv_weight_grad: float32 [3, 768, 768], P(None, None, 'mp')
- qv_bias_grad: float32 [2, 768], P(None, 'mp')
- out_weight_grad: float32 [768, 768], P('mp')
- out_bias_grad: float32 [768], replicated
- gain_two_grad: float32 [768], replicated
- shift_two_grad: float32 [768], replicated
- up_weight_grad: float32 [768, 3072], P(None, 'mp')
- up_bias_grad: float32 [3072], P('mp')
- down_weight_grad: float32 [3072, 768], P('mp')
- down_bias_grad: float32 [768], replicated
The draws below stay inside these ranges and needn't reach their ends.
Inputs may be any that keep to these rules, and one draw needn't show every extreme that they name: `segment_lengths`: each row sums to 512; its largest entry is 192.
All inputs are finite; a program needn't handle non-finite values.
Results may differ from the reference program's by a relative error of at most 0.014.
Values may be sent and summed in bfloat16 or wider, within the bound.
A program may use at most 192 MiB of HBM per device.

```python
import math
import jax
import jax.numpy as jnp
import numpy as np
from jax import lax

D = 768
HEADS = 12
HD = 64
FF = 3072
L = 512
NSEG = 8
SEQ_DEV = 4
MOST = 192
SEQS = 32
TOKENS = 16384
N_DP = 8


def draw_cotangent(key, part):
    base_key = jax.random.fold_in(jax.random.fold_in(key, 17), 0)
    fraction = jnp.arange(TOKENS, dtype=jnp.float32) / max(TOKENS - 1, 1)
    noise_part = jax.random.normal(base_key, (TOKENS, D), jnp.float32)
    values = noise_part * ((1.0 + 2.0 * fraction)[:, None] / 2.0)
    return jnp.clip(values, -8.0, 8.0).astype(jnp.bfloat16)


def level_of(own_key, shape, cuts, least, high):
    factor_of, own = 1.0, jax.random.fold_in(own_key, 6)
    for axis_at, blocks in cuts:
        heights = jnp.exp(jax.random.uniform(jax.random.fold_in(own, axis_at), (blocks,), jnp.float32, least / len(cuts), high / len(cuts)))
        factor_of = factor_of * jnp.repeat(heights, shape[axis_at] // blocks).reshape([-1 if axis == axis_at else 1 for axis in range(len(shape))])
    return factor_of


def split_up(amount, total, limit, slope):
    weights = [(1 << 20) // math.isqrt(standing ** slope) + 1 for standing in range(2, amount + 1)]
    spare, counts = total - limit - (amount - 1), [1] * (amount - 1)
    while spare > 0:
        free = [i for i in range(amount - 1) if counts[i] < limit]
        mass, left = sum([weights[i] for i in free]), spare
        for i in free:
            extra = min(limit - counts[i], max(1, left * weights[i] // mass), spare)
            counts[i] = counts[i] + extra
            spare = spare - extra
    return np.array([limit] + counts)


def ragged_sizes(stream_key, number_of, total, reach, skew):
    if number_of == 2:
        one = jax.random.randint(stream_key, (), max(1, total - reach), min(reach, total - 1) + 1)
        return jnp.stack([one, total - one])
    sizes = jnp.asarray(split_up(number_of, total, reach, skew), jnp.int32)
    twos = (number_of - 1) // 2
    giver, receiver = sizes[1:1 + 2 * twos:2], sizes[2:2 + 2 * twos:2]
    room = jnp.minimum(giver - 1, reach - receiver)
    passed = jax.random.randint(jax.random.fold_in(stream_key, 1), (twos,), 0, 1 << 20) % (room + 1)
    sizes = sizes.at[1:1 + 2 * twos:2].set(giver - passed).at[2:2 + 2 * twos:2].set(receiver + passed)
    return sizes[jax.random.permutation(jax.random.fold_in(stream_key, 2), number_of)]


def bell_draw(own_key, dims, width, limit, cuts=(), held_as=jnp.bfloat16):
    drawn = jax.random.normal(own_key, dims, jnp.float32) * width
    if len(cuts) > 0:
        drawn = level_of(own_key, dims, cuts, -0.22, 0.18) * drawn
    return jnp.clip(drawn, min=-limit, max=limit).astype(held_as)


def setup_inputs(seed: int = 0) -> dict:
    streams_of = jax.random.split(jax.random.key(seed), 16)
    tokens = bell_draw(streams_of[0], (TOKENS, D), 1.0, 6.0, ((0, 32),))
    segment_lengths = jax.vmap(lambda own: ragged_sizes(own, NSEG, L, MOST, 2))(jax.random.split(streams_of[1], SEQS)).reshape((SEQS, NSEG)).astype(jnp.int32)
    gain_one = jnp.clip(1.0 + 0.1 * jax.random.normal(streams_of[2], (D,), jnp.float32), 0.5, 1.5)
    shift_one = bell_draw(streams_of[3], (D,), 0.2, 1.25, (), jnp.float32)
    qkv_weight = bell_draw(streams_of[4], (3, D, D), D ** -0.5, 0.21875, ((2, 4),))
    qv_bias = bell_draw(streams_of[5], (2, D), 0.3, 1.75, ((1, 4),), jnp.float32)
    out_weight = bell_draw(streams_of[6], (D, D), (D // 32) ** -0.5, 1.25, ((0, 4),))
    out_bias = bell_draw(streams_of[7], (D,), 0.2, 1.25, (), jnp.float32)
    gain_two = jnp.clip(1.0 + 0.1 * jax.random.normal(streams_of[8], (D,), jnp.float32), 0.5, 1.5)
    shift_two = bell_draw(streams_of[9], (D,), 0.2, 1.25, (), jnp.float32)
    up_weight = bell_draw(streams_of[10], (D, FF), D ** -0.5, 0.21875, ((1, 4),))
    up_bias = bell_draw(streams_of[11], (FF,), 0.3, 1.75, ((0, 4),), jnp.float32)
    down_weight = bell_draw(streams_of[12], (FF, D), FF ** -0.5, 0.109375, ((0, 4),))
    down_bias = bell_draw(streams_of[13], (D,), 0.2, 1.25, (), jnp.float32)
    cotangent = draw_cotangent(jax.random.fold_in(streams_of[15], 71), 0)
    return {"tokens": tokens, "segment_lengths": segment_lengths, "gain_one": gain_one, "shift_one": shift_one, "qkv_weight": qkv_weight, "qv_bias": qv_bias, "out_weight": out_weight, "out_bias": out_bias, "gain_two": gain_two, "shift_two": shift_two, "up_weight": up_weight, "up_bias": up_bias, "down_weight": down_weight, "down_bias": down_bias, "cotangent": cotangent}


@jax.custom_vjp
def low(v):
    return lax.optimization_barrier(v.astype(jnp.bfloat16)).astype(jnp.float32)

@jax.custom_vjp
def low_back(v):
    return v

def low_keep(v):
    return (low(v), None)

def low_pass(kept, grad):
    return (grad,)

def back_keep(v):
    return (v, None)

def back_low(kept, grad):
    return (low(grad),)
low.defvjp(low_keep, low_pass)
low_back.defvjp(back_keep, back_low)

def norm_rows(values, gain_vec, bias_vec):
    row_mean = lax.optimization_barrier(jnp.mean(values, axis=-1, keepdims=True))
    centred = values - row_mean
    variance = lax.optimization_barrier(jnp.mean(centred * centred, axis=-1, keepdims=True))
    return centred * lax.rsqrt(variance + 1e-05) * gain_vec + bias_vec

def exact_gelu(values):
    return jax.nn.gelu(values, approximate=False)

def segment_ids(lengths):
    bounds = jnp.cumsum(lengths, axis=1)
    positions = jnp.arange(L, dtype=jnp.int32)
    return lax.optimization_barrier(jnp.sum((positions[None, :, None] >= bounds[:, None, :]).astype(jnp.int32), axis=2))

def forward_block(tok_rows, seg_ids, weights):
    gain_one, shift_one, qkv_weight, qv_bias, out_weight, out_bias, gain_two, shift_two, up_weight, up_bias, down_weight, down_bias = weights
    highest = lax.Precision.HIGHEST
    seq_count = seg_ids.shape[0]
    head_shape = (seq_count, L, HEADS, HD)
    normed_one = low(norm_rows(tok_rows, gain_one, shift_one))
    query_part = low(low_back(jnp.dot(normed_one, qkv_weight[0], precision=highest) + qv_bias[0]))
    key_part = low(low_back(jnp.dot(normed_one, qkv_weight[1], precision=highest)))
    value_part = low(low_back(jnp.dot(normed_one, qkv_weight[2], precision=highest) + qv_bias[1]))
    scores = jnp.einsum('sqhd,skhd->shqk', query_part.reshape(head_shape), key_part.reshape(head_shape), precision=highest) * (1.0 / math.sqrt(HD))
    same_segment = (seg_ids[:, :, None] == seg_ids[:, None, :])[:, None]
    scores = low_back(jnp.where(same_segment, scores, -1000000000.0))
    row_max = lax.optimization_barrier(jnp.max(scores, axis=-1, keepdims=True))
    shifted = jnp.exp(scores - row_max)
    softmax_weights = shifted / lax.optimization_barrier(jnp.sum(shifted, axis=-1, keepdims=True))
    attended = jnp.einsum('shqk,skhd->sqhd', low(softmax_weights), value_part.reshape(head_shape), precision=highest)
    keep_row = (seg_ids < NSEG - 1).astype(jnp.float32).reshape(seq_count * L, 1)
    attended = low(low_back(attended.reshape(seq_count * L, D) * keep_row))
    mixed_rows = tok_rows + low_back(jnp.dot(attended, out_weight, precision=highest)) + out_bias
    normed_two = low(norm_rows(mixed_rows, gain_two, shift_two))
    hidden = low_back(jnp.dot(normed_two, up_weight, precision=highest) + up_bias)
    active = low(exact_gelu(hidden))
    return mixed_rows + low_back(jnp.dot(active, down_weight, precision=highest)) + down_bias

def reference(tokens, segment_lengths, gain_one, shift_one, qkv_weight, qv_bias, out_weight, out_bias, gain_two, shift_two, up_weight, up_bias, down_weight, down_bias, cotangent):
    params = tuple((each_array.astype(jnp.float32) for each_array in (gain_one, shift_one, qkv_weight, qv_bias, out_weight, out_bias, gain_two, shift_two, up_weight, up_bias, down_weight, down_bias)))
    tok_blocks = tokens.astype(jnp.float32).reshape(N_DP, SEQ_DEV * L, D)
    cot_blocks = cotangent.astype(jnp.float32).reshape(N_DP, SEQ_DEV * L, D)
    id_blocks = segment_ids(segment_lengths).reshape(N_DP, SEQ_DEV, L)
    zero_grads = tuple((jnp.zeros_like(each_array) for each_array in params))

    def block_step(totals, inputs):
        tok_rows, cot_rows, seg_ids = inputs

        def local_forward(rows_in, weights):
            return forward_block(rows_in, seg_ids, weights)
        output, pullback = jax.vjp(local_forward, tok_rows, params)
        rows_grad, weight_grads = pullback(cot_rows)
        totals = tuple((first_sum + second_sum for first_sum, second_sum in zip(totals, weight_grads)))
        return (totals, (output, rows_grad))
    totals, (outputs, row_grads) = lax.scan(block_step, zero_grads, (tok_blocks, cot_blocks, id_blocks))
    layer_output = outputs.reshape(TOKENS, D)
    token_grad = row_grads.reshape(TOKENS, D)
    return (layer_output, token_grad, totals[0], totals[1], totals[2], totals[3], totals[4], totals[5], totals[6], totals[7], totals[8], totals[9], totals[10], totals[11])
```

```python
import functools
import math

import jax
import jax.numpy as jnp
from jax import lax
from jax.experimental import pallas as pl
from jax.experimental.pallas import tpu as pltpu
from jax.sharding import PartitionSpec as P

MESH = pl.DeviceIdType.MESH
F32, BF16 = jnp.float32, jnp.bfloat16
HD = 64
EPS = 1e-05
CHUNK = 128
INV_SQRT2 = 1.0 / math.sqrt(2.0)
INV_SQRT2PI = 1.0 / math.sqrt(2.0 * math.pi)


def dot(a, b, dims):
    return lax.dot_general(a, b, (dims, ((), ())), preferred_element_type=F32)


def nn(a, b):
    return dot(a, b, ((1,), (0,)))


def nt(a, b):
    return dot(a, b, ((1,), (1,)))


def tn(a, b):
    return dot(a, b, ((0,), (0,)))


def loop(n, fn):
    lax.fori_loop(0, n, lambda i, c: (fn(i), c)[1], 0)


def flip(value, bit):
    return value + bit * (1 - 2 * ((value // bit) % 2))


def body(
    n_dp,
    lens, tok, cot, g1, s1, ob, g2, s2, db, bias, wq_in, wo_in, wu_in, wd_in,
    lo, tg, gsum, small, wd_full,
    wq, wo, wu, wdbuf, biasg, n1, q, k, v, p, dsb, att, mixed, mg, n2, mgl, act, gp, mask,
    csend, crecv, xsend, keep, xrecv, yrecv, zrecv, fin, orecv, srecv,
    own_sem, ag_s, ag_r, b_s, b_r, wd_sem, c_s, c_r, credit, x_s, x_r, y_s, y_r, z_s, z_r,
    a_s, a_r, e_s, e_r, l_s, o_s, o_r, v_s, v_r,
):
    rows, d = tok.shape
    hw = wo_in.shape[0]
    ff = wu_in.shape[1]
    half_w = 2 * hw
    dp, mp = lax.axis_index("dp"), lax.axis_index("mp")
    x, c = mp // 2, mp % 2
    y, zz = dp % 2, dp // 2
    inner = min(n_dp, 8)
    nz = inner // 2
    n_out = n_dp // inner
    z1, zi, base = zz % 2, zz % nz, dp - dp % inner
    sib, xn = flip(mp, 1), flip(mp, 2)
    yn, zn = flip(dp, 1), flip(dp, 2)
    m_x, m_sx = xn, flip(xn, 1)
    groups = 3
    piece = CHUNK // 2 // nz
    per_group = d // CHUNK
    n_chunks = groups * per_group

    def rc(src, dst, ss, rs, dev):
        return pltpu.make_async_remote_copy(
            src_ref=src, dst_ref=dst, send_sem=ss, recv_sem=rs, device_id=dev, device_id_type=MESH
        )

    z_devs = [base + 2 * ((zi + o) % nz) + y for o in range(1, nz)]
    o_devs = [(dp + inner * o) % n_dp for o in range(1, n_out)]
    bits = [1 << b for b in range(n_dp.bit_length() - 1)]
    peers_dp = [yn] + z_devs + o_devs
    peers = [(dp, sib), (dp, xn), (dp, m_sx)] + [(e, mp) for e in peers_dp]

    barrier = pltpu.get_barrier_semaphore()
    for dev in peers:
        pl.semaphore_signal(barrier, inc=1, device_id=dev, device_id_type=MESH)
    pl.semaphore_wait(barrier, len(peers))

    quarter = [hw // 4, hw // 4, d // 4, ff // 4]

    def own(t, r0, n):
        if t == 0:
            return wq_in.at[:, pl.ds(r0, n), :]
        return (wo_in, wu_in, wd_in)[t - 1].at[pl.ds(r0, n), :]

    def full(t, m, r0, n):
        if t == 0:
            return wq.at[:, pl.ds(pl.multiple_of(m * hw + r0, 16), n), :]
        if t == 1:
            return wo.at[pl.ds(pl.multiple_of(m * hw + r0, 16), n), :]
        return (wu, wd_full)[t - 2].at[m, pl.ds(r0, n), :]

    q_own = y + 2 * z1
    q_y, q_z, q_d = (1 - y) + 2 * z1, y + 2 * (1 - z1), (1 - y) + 2 * (1 - z1)

    def reg(t, m, qq, part=None):
        n = quarter[t]
        r0 = pl.multiple_of(qq * n, 16)
        if part is None:
            return full(t, m, r0, n)
        if t == 0:
            ref = wq.at[pl.ds(0, 1)] if part == "y" else wq.at[pl.ds(1, 2)]
            return ref.at[:, pl.ds(pl.multiple_of(m * hw + r0, 16), n), :]
        if t == 1:
            return full(t, m, r0, n)
        return full(t, m, r0 + (0 if part == "y" else n // 2), n // 2)

    def whole(t, m):
        return full(t, m, 0, 4 * quarter[t])

    dev_s, dev_x, dev_y, dev_z = (dp, sib), (dp, xn), (yn, mp), (zn, mp)

    def c_own(t):
        return pltpu.make_async_copy(own(t, 0, 4 * quarter[t]), whole(t, mp), own_sem.at[t])

    def d_own(t):
        return rc(own(t, 0, 4 * quarter[t]), whole(t, mp), ag_s.at[t, 0], ag_r.at[t, 0], dev_s)

    def d_x(t):
        n = quarter[t]
        return rc(own(t, pl.multiple_of(q_own * n, 16), n), reg(t, mp, q_own), ag_s.at[t, 1], ag_r.at[t, 1], dev_x)

    def fwd(t, qq, part, si, ri, dev):
        r = reg(t, m_x, qq, part)
        return rc(r, r, ag_s.at[t, si], ag_r.at[t, ri], dev)

    def d_y(t):
        return fwd(t, q_own, None, 2, 2, dev_y)

    def d_z(t):
        return fwd(t, q_own, None, 3, 3, dev_z)

    def d_s(t, qq, si):
        return fwd(t, qq, None, si, 6, dev_s)

    def d_dz(t):
        return fwd(t, q_y, "z", 6, 4, dev_z)

    def d_dy(t):
        return fwd(t, q_z, "y", 8, 5, dev_y)

    def arrive(region, sem, dev):
        rc(region, region, ag_s.at[0, 0], sem, dev).wait_recv()

    def f1(t):
        arrive(reg(t, m_x, q_own), ag_r.at[t, 1], dev_x)
        d_y(t).start()
        d_z(t).start()
        d_s(t, q_own, 4).start()

    def f2(t):
        arrive(reg(t, m_x, q_y), ag_r.at[t, 2], dev_y)
        if t != 1:
            d_dz(t).start()
        d_s(t, q_y, 5).start()
        arrive(reg(t, m_x, q_z), ag_r.at[t, 3], dev_z)
        d_dy(t).start()
        d_s(t, q_z, 7).start()

    def f3(t):
        if t != 1:
            arrive(reg(t, m_x, q_d, "z"), ag_r.at[t, 4], dev_z)
        arrive(reg(t, m_x, q_d, "y"), ag_r.at[t, 5], dev_y)
        d_s(t, q_d, 9).start()

    def near(t):
        c_own(t).wait()
        arrive(whole(t, sib), ag_r.at[t, 0], dev_s)

    def far(t):
        arrive(whole(t, m_sx), ag_r.at[t, 6], dev_s)

    def sent(t):
        for cp in (d_own(t), d_x(t), d_y(t), d_z(t), d_s(t, q_own, 4), d_s(t, q_y, 5), d_s(t, q_z, 7),
                   d_dy(t), d_s(t, q_d, 9)):
            cp.wait_send()
        if t != 1:
            d_dz(t).wait_send()

    def d_bias(i):
        dev = [sib, xn, m_sx][i]
        return rc(bias, biasg.at[mp], b_s.at[i], b_r.at[i], (dp, dev))

    for t in range(4):
        d_x(t).start()
        d_own(t).start()
        c_own(t).start()
        if t == 0:
            for i in range(3):
                d_bias(i).start()

    def rows_of(ref, r0, n):
        return ref.at[pl.ds(pl.multiple_of(r0, 16), n), :]

    half = CHUNK // 2

    def d_xs(t):
        return rc(rows_of(xsend, t * CHUNK, CHUNK), rows_of(xrecv, t * CHUNK, CHUNK), x_s.at[t], x_r.at[t], dev_x)

    def d_ys(t):
        return rc(rows_of(keep, t * CHUNK + (1 - y) * half, half), rows_of(yrecv, t * half, half),
                  y_s.at[t], y_r.at[t], dev_y)

    def piece_at(t, zj):
        return t * CHUNK + y * half + zj * piece

    def d_zs(t, o):
        j = t * (nz - 1) + o - 1
        return rc(rows_of(keep, piece_at(t, (zi + o) % nz), piece), rows_of(zrecv, j * piece, piece),
                  z_s.at[j], z_r.at[j], (z_devs[o - 1], mp))

    def d_as(t, o):
        j = t * (nz - 1) + o - 1
        return rc(rows_of(fin, t * piece, piece), rows_of(gsum, piece_at(t, zi), piece),
                  a_s.at[j], a_r.at[j], (z_devs[o - 1], mp))

    def d_ar(t, o):
        j = t * (nz - 1) + o - 1
        r = rows_of(gsum, piece_at(t, (zi + nz - o) % nz), piece)
        return rc(r, r, a_s.at[j], a_r.at[j], (z_devs[o - 1], mp))

    def d_os(t, o):
        j = t * (n_out - 1) + o - 1
        return rc(rows_of(fin, t * piece, piece), rows_of(orecv, j * piece, piece),
                  o_s.at[j], o_r.at[j], (o_devs[o - 1], mp))

    def c_ls(t):
        return pltpu.make_async_copy(rows_of(fin, t * piece, piece), rows_of(gsum, piece_at(t, zi), piece), l_s.at[t])

    def d_es(t):
        r = rows_of(gsum, t * CHUNK + y * half, half)
        return rc(r, r, e_s.at[t], e_r.at[t], dev_y)

    def d_er(t):
        r = rows_of(gsum, t * CHUNK + (1 - y) * half, half)
        return rc(r, r, e_s.at[t], e_r.at[t], dev_y)

    def get(ref, r0, n):
        return ref[pl.ds(pl.multiple_of(r0, 16), n), :].astype(F32)

    def put(ref, r0, n, val):
        ref[pl.ds(pl.multiple_of(r0, 16), n), :] = val.astype(BF16)

    def st_y(t):
        d_xs(t).wait_recv()
        r0 = t * CHUNK
        put(keep, r0, CHUNK, get(keep, r0, CHUNK) + get(xrecv, r0, CHUNK))
        d_ys(t).start()

    def st_z(t):
        d_ys(t).wait_recv()
        r0 = t * CHUNK + y * half
        put(keep, r0, half, get(keep, r0, half) + get(yrecv, t * half, half))
        for o in range(1, nz):
            d_zs(t, o).start()

    def st_a(t):
        for o in range(1, nz):
            d_zs(t, o).wait_recv()
        acc = get(keep, piece_at(t, zi), piece)
        for o in range(1, nz):
            acc = acc + get(zrecv, (t * (nz - 1) + o - 1) * piece, piece)
        put(fin, t * piece, piece, acc)
        if n_out == 1:
            st_g(t)
        else:
            for o in range(1, n_out):
                d_os(t, o).start()

    def st_o(t):
        own_part = get(fin, t * piece, piece)
        acc = own_part
        for o in range(1, n_out):
            d_os(t, o).wait_recv()
            d_os(t, o).wait_send()
        me = dp // inner
        acc = jnp.zeros_like(own_part)
        for gidx in range(n_out):
            slot = (me - gidx + n_out) % n_out
            r0 = (t * (n_out - 1) + jnp.maximum(slot, 1) - 1) * piece
            acc = acc + jnp.where(slot == 0, own_part, get(orecv, r0, piece))
        put(fin, t * piece, piece, acc)
        st_g(t)

    def st_g(t):
        c_ls(t).start()
        for o in range(1, nz):
            d_as(t, o).start()

    def st_b(t):
        c_ls(t).wait()
        for o in range(1, nz):
            d_ar(t, o).wait_recv()
        d_es(t).start()

    def st_e(t):
        d_er(t).wait_recv()
        d_xs(t).wait_send()
        d_ys(t).wait_send()
        d_es(t).wait_send()
        for o in range(1, nz):
            d_zs(t, o).wait_send()
            d_as(t, o).wait_send()

    stages = [st_y, st_z, st_a] + ([st_o] if n_out > 1 else []) + [st_b, st_e]

    def tick(t):
        for s in reversed(range(len(stages))):
            u = t - s

            @pl.when(jnp.logical_and(u >= 0, u < n_chunks))
            def _(s=s, u=u):
                stages[s](u)

    def d_c(slot):
        return rc(csend.at[slot], crecv.at[slot], c_s.at[slot], c_r.at[slot], dev_s)

    def m_of(i):
        mx = jnp.where(i % 2 == 0, 1 - x, x)
        mc = jnp.where(i < 2, 1 - c, c)
        return 2 * mx + mc

    small[...] = jnp.zeros_like(small)
    rb = 128

    def ln1(i):
        r = pl.ds(pl.multiple_of(i * rb, rb), rb)
        xv = tok[r, :].astype(F32)
        xc = xv - jnp.mean(xv, axis=-1, keepdims=True)
        inv = lax.rsqrt(jnp.mean(xc * xc, axis=-1, keepdims=True) + EPS)
        n1[r, :] = (xc * inv * g1[...] + s1[...]).astype(BF16)
        small[5:6, :] += jnp.sum(cot[r, :].astype(F32), axis=0, keepdims=True)

    loop(rows // rb, ln1)

    n_seg = lens.shape[1]
    col = lax.broadcasted_iota(jnp.int32, (rows, 1), 0)
    row = lax.broadcasted_iota(jnp.int32, (1, rows), 1)
    seg_col, seg_row = jnp.zeros_like(col), jnp.zeros_like(row)
    bound = jnp.int32(0)
    for j in range(n_seg):
        bound = bound + lens[mp, j]
        seg_col = seg_col + (col >= bound).astype(jnp.int32)
        seg_row = seg_row + (row >= bound).astype(jnp.int32)
    mask[...] = jnp.where(seg_col == seg_row, 0.0, -1000000000.0).astype(F32)
    kept = (seg_col < n_seg - 1).astype(F32)

    biasg[mp] = bias[...]
    for i in range(3):
        d_bias(i).wait()
    bias_sum = biasg[0, 1:3, :] + biasg[1, 1:3, :] + biasg[2, 1:3, :] + biasg[3, 1:3, :]
    small[14:16, :] = bias_sum

    scale = 1.0 / math.sqrt(HD)
    n_pairs = d // (2 * HD)
    per_half = n_pairs // 2
    low_half = lax.broadcasted_iota(jnp.int32, (1, 2 * HD), 1) < HD
    ab = rows // 2

    def lanes_of(i):
        xh = jnp.where(i < per_half, x, 1 - x)
        pair = xh * per_half + i % per_half
        return xh, pair, pl.ds(pl.multiple_of(pair * 2 * HD, 128), 2 * HD)

    def pick(h, val):
        zero = jnp.zeros_like(val)
        return jnp.where(low_half, val, zero) if h == 0 else jnp.where(low_half, zero, val)

    def attn_fwd(i):
        xh, pair, lanes = lanes_of(i)

        @pl.when(i == 0)
        def _():
            near(0)

        @pl.when(i == per_half)
        def _():
            far(0)

        @pl.when(i % per_half == 0)
        def _():
            w_rows = pl.ds(pl.multiple_of(xh * half_w, 128), half_w)
            w_lanes = w_rows
            for cc, ref in enumerate((q, k, v)):
                val = nt(n1[...], wq[cc, w_rows, :])
                if cc == 0:
                    val = val + small[14:15, w_lanes]
                if cc == 2:
                    val = val + small[15:16, w_lanes]
                val = val.astype(BF16)
                if cc == 0:
                    val = val * jnp.asarray(scale, BF16)
                ref[:, w_lanes] = val

        k2, v2 = k[:, lanes], v[:, lanes]
        for r in range(2):
            rs = pl.ds(r * ab, ab)
            q2 = q[rs, lanes]
            outs = []
            for h in range(2):
                sc = nt(pick(h, q2), k2) + mask[rs, :]
                e = jnp.exp(sc - jnp.max(sc, axis=-1, keepdims=True))
                pr = (e * (1.0 / jnp.sum(e, axis=-1, keepdims=True))).astype(BF16)
                p[2 * pair + h, rs, :] = pr
                outs.append(nn(pr, v2))
            o2 = jnp.where(low_half, outs[0], outs[1]) * kept[r * ab:(r + 1) * ab]
            att[rs, lanes] = o2.astype(BF16)

        for at, todo in enumerate(AG_PLAN):
            @pl.when(i == at)
            def _(todo=todo):
                for fn, t in todo:
                    (f1, f2, f3)[fn - 1](t)

    AG_PLAN = [
        [(1, 0)],
        [(2, 0), (1, 1)],
        [(3, 0), (2, 1), (1, 2)],
        [(3, 1), (2, 2), (1, 3)],
        [(3, 2), (2, 3)],
        [(3, 3)],
    ]
    loop(n_pairs, attn_fwd)

    near(1)
    far(1)
    mixed[...] = nn(att[...], wo[...])

    def ln2(i):
        r = pl.ds(pl.multiple_of(i * rb, rb), rb)
        xv = tok[r, :].astype(F32) + mixed[r, :] + ob[...]
        mixed[r, :] = xv
        lo[r, :] = xv + db[...]
        xc = xv - jnp.mean(xv, axis=-1, keepdims=True)
        inv = lax.rsqrt(jnp.mean(xc * xc, axis=-1, keepdims=True) + EPS)
        n2[r, :] = (xc * inv * g2[...] + s2[...]).astype(BF16)

    loop(rows // rb, ln2)

    tile = 256

    def emit_block(g, i, make):
        if g > 0:
            @pl.when(i < 2)
            def _():
                pl.semaphore_wait(credit.at[i], 1)
                d_c(i).wait_send()

        @pl.when(i >= 2)
        def _():
            d_c(i - 2).wait_recv()

        def part(r):
            rr = pl.ds(pl.multiple_of(r * tile, tile), tile)
            res = make(r)

            @pl.when(i < 2)
            def _():
                csend[i, rr, :] = res.astype(BF16)

            @pl.when(i >= 2)
            def _():
                tot = (res + crecv[i - 2, rr, :].astype(F32)).astype(BF16)
                out = pl.ds(pl.multiple_of(g * d + r * tile, tile), tile)

                @pl.when(i == 2)
                def _():
                    xsend[out, :] = tot
                    for cc in range(tile // CHUNK):
                        d_xs(g * per_group + r * (tile // CHUNK) + cc).start()

                @pl.when(i == 3)
                def _():
                    keep[out, :] = tot

        loop(d // tile, part)

        @pl.when(i < 2)
        def _():
            d_c(i).start()

        @pl.when(i >= 2)
        def _():
            pl.semaphore_signal(credit.at[i - 2], inc=1, device_id=dev_s, device_id_type=MESH)

    near(2)
    far(2)

    def ffn1(i):
        m = m_of(i)

        def hid(n):
            nl = pl.ds(pl.multiple_of(n * tile, tile), tile)
            h = nn(n2[...], wu[m, :, nl]) + biasg[m, 0:1, nl]
            phi = 0.5 * (1.0 + lax.erf(h * INV_SQRT2))
            act[m, :, nl] = (h * phi).astype(BF16)
            gp[m, :, nl] = (phi + h * jnp.exp(-0.5 * h * h) * INV_SQRT2PI).astype(BF16)

        loop(ff // tile, hid)

        def make(r):
            rl = pl.ds(pl.multiple_of(r * tile, tile), tile)
            return tn(act[m, :, rl], cot[...])

        emit_block(0, i, make)

    loop(4, ffn1)

    near(3)
    far(3)

    def c_wd(i):
        return pltpu.make_async_copy(wd_full.at[m_of(i)], wdbuf.at[i % 2], wd_sem.at[i % 2])

    c_wd(0).start()
    mg[...] = jnp.zeros_like(mg)

    def ffn2(i):
        m = m_of(i)
        c_wd(i).wait()

        @pl.when(i < 3)
        def _():
            c_wd(i + 1).start()

        s = i % 2

        def hg(n):
            nl = pl.ds(pl.multiple_of(n * tile, tile), tile)
            val = (gp[m, :, nl].astype(F32) * nt(cot[...], wdbuf[s, nl, :])).astype(BF16)
            gp[m, :, nl] = val
            small[pl.ds(8 + m, 1), nl] = jnp.sum(val.astype(F32), axis=0, keepdims=True)

        loop(ff // tile, hg)

        def make(r):
            rl = pl.ds(pl.multiple_of(r * tile, tile), tile)
            return tn(n2[:, rl], gp[m])

        emit_block(1, i, make)

        def back(n):
            nl = pl.ds(pl.multiple_of(n * tile, tile), tile)
            mg[:, nl] += nt(gp[m], wu[m, nl, :])
            lo[:, nl] += nn(act[m], wdbuf[s, :, nl])

        loop(d // tile, back)
        tick(i)

    loop(4, ffn2)

    def ln2b(i):
        r = pl.ds(pl.multiple_of(i * rb, rb), rb)
        xv = mixed[r, :]
        xc = xv - jnp.mean(xv, axis=-1, keepdims=True)
        inv = lax.rsqrt(jnp.mean(xc * xc, axis=-1, keepdims=True) + EPS)
        xh = xc * inv
        dn = mg[r, :]
        small[2:3, :] += jnp.sum(dn * xh, axis=0, keepdims=True)
        small[3:4, :] += jnp.sum(dn, axis=0, keepdims=True)
        gg = dn * g2[...]
        val = cot[r, :].astype(F32) + (
            gg - jnp.mean(gg, axis=-1, keepdims=True) - xh * jnp.mean(gg * xh, axis=-1, keepdims=True)
        ) * inv
        mg[r, :] = val
        mgl[r, :] = val.astype(BF16)
        small[4:5, :] += jnp.sum(val, axis=0, keepdims=True)

    loop(rows // rb, ln2b)

    da = n2

    def dab(n):
        nl = pl.ds(pl.multiple_of(n * tile, tile), tile)
        da[:, nl] = (nt(mgl[...], wo[nl, :]).astype(BF16).astype(F32) * kept).astype(BF16)

    loop(d // tile, dab)
    tick(4)

    def attn_bwd(i):
        xh, pair, lanes = lanes_of((i + per_half) % n_pairs)
        k2, v2 = k[:, lanes], v[:, lanes]
        do2, q2 = da[:, lanes], q[:, lanes]
        dqs, dks, dvs = [], [], []
        for h in range(2):
            dq_rows = []
            for r in range(2):
                rs = slice(r * ab, (r + 1) * ab)
                dpv = nt(pick(h, do2[rs]), v2)
                pr = p[2 * pair + h, pl.ds(r * ab, ab), :].astype(F32)
                t1 = pr * dpv
                ds = (t1 - pr * jnp.sum(t1, axis=-1, keepdims=True)).astype(BF16)
                dsb[pl.ds(r * ab, ab), :] = ds
                dq_rows.append(nn(ds, k2))
            dqs.append(jnp.concatenate(dq_rows, axis=0))
            dks.append(tn(dsb[...], q2))
            dvs.append(tn(p[2 * pair + h], do2))
        dv2 = jnp.where(low_half, dvs[0], dvs[1]).astype(BF16)
        dk2 = jnp.where(low_half, dks[0], dks[1]).astype(BF16)
        dq2 = (jnp.where(low_half, dqs[0], dqs[1]) * scale).astype(BF16)
        q[:, lanes] = dq2
        k[:, lanes] = dk2
        v[:, lanes] = dv2
        small[6:7, lanes] = jnp.sum(dq2.astype(F32), axis=0, keepdims=True)
        small[7:8, lanes] = jnp.sum(dv2.astype(F32), axis=0, keepdims=True)

        @pl.when(i % per_half == per_half - 1)
        def _():
            a = i // per_half
            wl = pl.ds(pl.multiple_of(xh * half_w, 128), half_w)
            pl.semaphore_wait(credit.at[a], 1)
            d_c(a).wait_send()
            for j, (ref, other) in enumerate(((att, mgl), (q, n1), (k, n1), (v, n1))):
                act[pl.ds(0, 2), pl.ds(0, hw), :] = tn(ref[:, wl], other[...]).astype(BF16).reshape(2, hw, d)
                csend[a, j * hw:(j + 1) * hw, :] = act[1 - c, 0:hw, :]
                gp[0 if j < 2 else 1, (j % 2) * hw:(j % 2 + 1) * hw, :] = act[c, 0:hw, :]
            d_c(a).start()
            d_c(a).wait_recv()
            for j in range(4):
                tot = (gp[0 if j < 2 else 1, (j % 2) * hw:(j % 2 + 1) * hw, :].astype(F32)
                       + crecv[a, j * hw:(j + 1) * hw, :].astype(F32)).astype(BF16)

                @pl.when(a == 0)
                def _():
                    xsend[2 * d + j * hw:2 * d + (j + 1) * hw, :] = tot

                @pl.when(a == 1)
                def _():
                    keep[2 * d + j * hw:2 * d + (j + 1) * hw, :] = tot

            @pl.when(a == 0)
            def _():
                for cc in range(per_group):
                    d_xs(2 * per_group + cc).start()

        tick(5 + i)

    loop(n_pairs, attn_bwd)

    def ln1n(n):
        nl = pl.ds(pl.multiple_of(n * tile, tile), tile)
        tg[:, nl] = nn(q[...], wq[0, :, nl]) + nn(k[...], wq[1, :, nl]) + nn(v[...], wq[2, :, nl])

    loop(d // tile, ln1n)

    def ln1b(i):
        r = pl.ds(pl.multiple_of(i * rb, rb), rb)
        xv = tok[r, :].astype(F32)
        xc = xv - jnp.mean(xv, axis=-1, keepdims=True)
        inv = lax.rsqrt(jnp.mean(xc * xc, axis=-1, keepdims=True) + EPS)
        xh = xc * inv
        dn = tg[r, :]
        small[0:1, :] += jnp.sum(dn * xh, axis=0, keepdims=True)
        small[1:2, :] += jnp.sum(dn, axis=0, keepdims=True)
        gg = dn * g1[...]
        tg[r, :] = mg[r, :] + (
            gg - jnp.mean(gg, axis=-1, keepdims=True) - xh * jnp.mean(gg * xh, axis=-1, keepdims=True)
        ) * inv

    loop(rows // rb, ln1b)

    v_devs = [(dp, sib), (dp, xn)] + [(flip(dp, b), mp) for b in bits]

    def d_v(s):
        return rc(small, srecv.at[s], v_s.at[s], v_r.at[s], v_devs[s])

    first = 5 + n_pairs

    def tail(i):
        for s in range(len(v_devs) + 1):
            @pl.when(i == s)
            def _(s=s):
                if s > 0:
                    d_v(s - 1).wait()
                    small[...] += srecv[s - 1]
                if s < len(v_devs):
                    d_v(s).start()

        tick(first + i)

    loop(max(n_chunks + len(stages) - 1 - first, len(v_devs) + 1), tail)
    for slot in range(2):
        d_c(slot).wait_send()
    for t in range(4):
        sent(t)


def layer(n_dp, tokens, lens, g1, s1, wqkv, qvb, wo, ob, g2, s2, wu, ub, wd, db, cot):
    rows, d = tokens.shape
    hw, ff = wo.shape[0], wu.shape[1]
    n_mp = lax.axis_size("mp")
    mp = lax.axis_index("mp")
    inner = min(n_dp, 8)
    nz, n_out = inner // 2, n_dp // inner
    piece = CHUNK // 2 // nz
    nc = 3 * d // CHUNK
    n_small = 2 + n_dp.bit_length() - 1
    heads = d // HD
    vec = lambda a: a.reshape(1, d)
    lane = jnp.arange(d, dtype=jnp.int32)[None, :]
    wide = jnp.concatenate([qvb] * n_mp, axis=1)
    bias = jnp.concatenate(
        [ub.reshape(1, d), jnp.where(lane // hw == mp, wide, 0.0), jnp.zeros((5, d), F32)], axis=0
    )
    wqt = jnp.swapaxes(wqkv, 1, 2)
    vm = pl.BlockSpec(memory_space=pltpu.VMEM)
    hbm = pl.BlockSpec(memory_space=pl.ANY)
    sm = pl.BlockSpec(memory_space=pltpu.SMEM)
    dma = pltpu.SemaphoreType.DMA
    S = jax.ShapeDtypeStruct
    V = pltpu.VMEM
    nzr = max(nc * (nz - 1), 1)
    nor = max(nc * (n_out - 1), 1)
    lo, tg, gsum, small, _ = pl.pallas_call(
        functools.partial(body, n_dp),
        out_shape=(
            S((rows, d), F32), S((rows, d), F32), S((3 * d, d), BF16), S((16, d), F32), S((n_mp, ff, d), BF16),
        ),
        in_specs=[sm] + [vm] * 9 + [hbm] * 4,
        out_specs=(vm, vm, hbm, vm, hbm),
        scratch_shapes=[
            V((3, d, d), BF16), V((d, d), BF16), V((n_mp, d, ff), BF16), V((2, ff, d), BF16), V((n_mp, 8, d), F32),
            V((rows, d), BF16), V((rows, d), BF16), V((rows, d), BF16), V((rows, d), BF16),
            V((heads, rows, rows), BF16), V((rows, rows), BF16), V((rows, d), BF16),
            V((rows, d), F32), V((rows, d), F32), V((rows, d), BF16), V((rows, d), BF16),
            V((n_mp, rows, ff), BF16), V((n_mp, rows, ff), BF16), V((rows, rows), F32),
            V((2, d, d), BF16), V((2, d, d), BF16), V((3 * d, d), BF16), V((3 * d, d), BF16), V((3 * d, d), BF16),
            V((nc * CHUNK // 2, d), BF16), V((nzr * piece, d), BF16), V((nc * piece, d), BF16),
            V((nor * piece, d), BF16), V((n_small, 16, d), F32),
            dma((4,)), dma((4, 10)), dma((4, 7)), dma((3,)), dma((3,)), dma((2,)), dma((2,)), dma((2,)),
            pltpu.SemaphoreType.REGULAR((2,)), dma((nc,)), dma((nc,)), dma((nc,)), dma((nc,)),
            dma((nzr,)), dma((nzr,)), dma((nzr,)), dma((nzr,)), dma((nc,)), dma((nc,)), dma((nc,)),
            dma((nor,)), dma((nor,)), dma((n_small,)), dma((n_small,)),
        ],
        compiler_params=pltpu.CompilerParams(
            collective_id=0, has_side_effects=True, vmem_limit_bytes=67043328
        ),
        name="layer",
    )(lens, tokens, cot, vec(g1), vec(s1), vec(ob), vec(g2), vec(s2), vec(db), bias, wqt, wo, wu, wd)

    f = lambda a: a.astype(F32)
    dqkv = f(jnp.swapaxes(gsum[2 * d + hw:].reshape(3, hw, d), 1, 2))
    qv = lax.dynamic_slice(small, (6, mp * hw), (2, hw))
    upb = lax.dynamic_slice(small, (8 + mp, 0), (1, d)).reshape(d)
    return (
        lo, tg, small[0], small[1], dqkv, qv, f(gsum[2 * d:2 * d + hw]), small[4], small[2], small[3],
        f(gsum[d:2 * d]), upb, f(gsum[:d]), small[5],
    )


def solution(mesh):
    rows = P(("dp", "mp"), None)
    in_specs = (
        rows, P("dp", None), P(), P(), P(None, None, "mp"), P(None, "mp"), P("mp", None), P(), P(), P(),
        P(None, "mp"), P("mp"), P("mp", None), P(), rows,
    )
    out_specs = (
        rows, rows, P(), P(), P(None, None, "mp"), P(None, "mp"), P("mp", None), P(), P(), P(),
        P(None, "mp"), P("mp"), P("mp", None), P(),
    )
    return jax.shard_map(
        functools.partial(layer, mesh.shape["dp"]), mesh=mesh, in_specs=in_specs, out_specs=out_specs, check_vma=False
    )
```

```python
import functools
import math

import jax
import jax.numpy as jnp
from jax import lax
from jax.experimental import pallas as pl
from jax.experimental.pallas import tpu as pltpu
from jax.sharding import PartitionSpec as P

MESH = pl.DeviceIdType.MESH
F32, BF16 = jnp.float32, jnp.bfloat16
HD = 64
EPS = 1e-05
CHUNK = 128
INV_SQRT2 = 1.0 / math.sqrt(2.0)
INV_SQRT2PI = 1.0 / math.sqrt(2.0 * math.pi)


def dot(a, b, dims):
    return lax.dot_general(a, b, (dims, ((), ())), preferred_element_type=F32)


def nn(a, b):
    return dot(a, b, ((1,), (0,)))


def nt(a, b):
    return dot(a, b, ((1,), (1,)))


def tn(a, b):
    return dot(a, b, ((0,), (0,)))


def loop(n, fn):
    lax.fori_loop(0, n, lambda i, c: (fn(i), c)[1], 0)


def flip(value, bit):
    return value + bit * (1 - 2 * ((value // bit) % 2))


def body(
    n_dp,
    lens, tok_in, cot_in, g1, s1, ob, g2, s2, db, ub_in, qvb_in, wq_in, wo_in, wu_in, wd_in,
    lo_out, tg_out, gsum, small, wd_full,
    tok, cot, lo, tg, bias, vecs, qvb,
    wq, wo, wu, wdbuf, biasg, n1, q, k, v, p, dsb, att, mixed, mg, n2, mgl, act, gp, mask,
    csend, crecv, xsend, keep, xrecv, yrecv, zrecv, fin, orecv, srecv,
    io_sem, own_sem, own_s, own_r, far_r, ag_s, ag_r, b_s, b_r, wd_sem, c_s, c_r, credit, x_s, x_r, y_s, y_r, z_s, z_r,
    a_s, a_r, e_s, e_r, l_s, o_s, o_r, v_s, v_r,
):
    rows, d = tok.shape
    c_tok = pltpu.make_async_copy(tok_in, tok, io_sem.at[0])
    c_cot = pltpu.make_async_copy(cot_in, cot, io_sem.at[1])
    c_lo = pltpu.make_async_copy(lo, lo_out, io_sem.at[2])
    c_tg = pltpu.make_async_copy(tg, tg_out, io_sem.at[3])
    c_tok.start()
    c_cot.start()
    hw = wo_in.shape[0]
    ff = wu_in.shape[1]
    half_w = 2 * hw
    dp, mp = lax.axis_index("dp"), lax.axis_index("mp")
    x, c = mp // 2, mp % 2
    y, zz = dp % 2, dp // 2
    inner = min(n_dp, 8)
    nz = inner // 2
    n_out = n_dp // inner
    z1, zi, base = zz % 2, zz % nz, dp - dp % inner
    sib, xn = flip(mp, 1), flip(mp, 2)
    yn, zn = flip(dp, 1), flip(dp, 2)
    m_x, m_sx = xn, flip(xn, 1)
    groups = 3
    piece = CHUNK // 2 // nz
    per_group = d // CHUNK
    n_chunks = groups * per_group

    def rc(src, dst, ss, rs, dev):
        return pltpu.make_async_remote_copy(
            src_ref=src, dst_ref=dst, send_sem=ss, recv_sem=rs, device_id=dev, device_id_type=MESH
        )

    z_devs = [base + 2 * ((zi + o) % nz) + y for o in range(1, nz)]
    o_devs = [(dp + inner * o) % n_dp for o in range(1, n_out)]
    bits = [1 << b for b in range(n_dp.bit_length() - 1)]
    peers_dp = [yn] + z_devs + o_devs
    peers = [(dp, sib), (dp, xn), (dp, m_sx)] + [(e, mp) for e in peers_dp]

    bias[...] = jnp.zeros_like(bias)
    bias[0:1, :] = ub_in[...].reshape(1, d)
    bias[1:3, 0:hw] = qvb_in[...]
    for n, ref in enumerate((g1, s1, ob, g2, s2, db)):
        vecs[n:n + 1, :] = ref[...].reshape(1, d)
    g1, s1, ob, g2, s2, db = (vecs.at[pl.ds(n, 1)] for n in range(6))
    barrier = pltpu.get_barrier_semaphore()
    for dev in peers:
        pl.semaphore_signal(barrier, inc=1, device_id=dev, device_id_type=MESH)
    pl.semaphore_wait(barrier, len(peers))

    n_units = 12
    quarter = hw // 4

    def own(u, r0, n):
        if u < 3:
            return wq_in.at[u, pl.ds(r0, n), :]
        if u == 3:
            return wo_in.at[pl.ds(r0, n), :]
        return (wu_in if u < 8 else wd_in).at[pl.ds((u % 4) * hw + r0, n), :]

    def full(u, m, r0, n):
        if u < 4:
            return (wq.at[u] if u < 3 else wo).at[pl.ds(pl.multiple_of(m * hw + r0, 16), n), :]
        return (wu if u < 8 else wd_full).at[m, pl.ds((u % 4) * hw + r0, n), :]

    q_own = y + 2 * z1
    q_y, q_z, q_d = (1 - y) + 2 * z1, y + 2 * (1 - z1), (1 - y) + 2 * (1 - z1)

    def start_of(qq):
        return pl.multiple_of(qq * quarter, 16)

    def reg(u, m, qq):
        return full(u, m, start_of(qq), quarter)

    def shard_in(t):
        return (wq_in, wo_in, wu_in, wd_in)[t]

    def whole(t, m):
        if t == 0:
            return wq.at[:, pl.ds(pl.multiple_of(m * hw, 16), hw), :]
        if t == 1:
            return wo.at[pl.ds(pl.multiple_of(m * hw, 16), hw), :]
        return (wu, wd_full)[t - 2].at[m]

    def tensor_of(u):
        return 0 if u < 3 else 1 if u == 3 else 2 if u < 8 else 3

    def kind(u):
        return "x" if u < 4 else "yz"[u % 2]

    dev_s, dev_x, dev_y, dev_z = (dp, sib), (dp, xn), (yn, mp), (zn, mp)

    def c_own(t):
        return pltpu.make_async_copy(shard_in(t), whole(t, mp), own_sem.at[t])

    def d_own(t):
        return rc(shard_in(t), whole(t, mp), own_s.at[t], own_r.at[t], dev_s)

    def d_x(u):
        return rc(own(u, start_of(q_own), quarter), reg(u, mp, q_own), ag_s.at[u, 0], ag_r.at[u, 0], dev_x)

    def d_xd(u):
        return rc(own(u, start_of(q_d), quarter), reg(u, mp, q_d), ag_s.at[u, 1], ag_r.at[u, 1], dev_x)

    def fwd(u, qq, si, rs, dev):
        r = reg(u, m_x, qq)
        return rc(r, r, ag_s.at[u, si], rs, dev)

    def d_y(u):
        return fwd(u, q_own, 2, ag_r.at[u, 2], dev_y)

    def d_z(u):
        return fwd(u, q_own, 3, ag_r.at[u, 3], dev_z)

    def d_s(u, qq, si):
        return fwd(u, qq, si, far_r.at[tensor_of(u)], dev_s)

    def d_dg(u):
        if kind(u) == "y":
            return fwd(u, q_z, 1, ag_r.at[u, 1], dev_y)
        return fwd(u, q_y, 1, ag_r.at[u, 1], dev_z)

    def arrive(region, sem, dev):
        rc(region, region, ag_s.at[0, 0], sem, dev).wait_recv()

    def f1(u):
        arrive(reg(u, m_x, q_own), ag_r.at[u, 0], dev_x)
        d_y(u).start()
        d_z(u).start()
        d_s(u, q_own, 4).start()

    def f2(u):
        arrive(reg(u, m_x, q_y), ag_r.at[u, 2], dev_y)
        arrive(reg(u, m_x, q_z), ag_r.at[u, 3], dev_z)
        if kind(u) != "x":
            d_dg(u).start()
        d_s(u, q_y, 5).start()
        d_s(u, q_z, 6).start()

    def f3(u):
        arrive(reg(u, m_x, q_d), ag_r.at[u, 1], {"x": dev_x, "y": dev_y, "z": dev_z}[kind(u)])
        d_s(u, q_d, 7).start()

    def do(*todo):
        for step, u in todo:
            (f1, f2, f3)[step - 1](u)

    def near(t):
        if t < 3:
            c_own(t).wait()
        arrive(whole(t, sib), own_r.at[t], dev_s)

    def far(t):
        arrive(whole(t, m_sx), far_r.at[t], dev_s)

    def sent():
        for t in range(4):
            d_own(t).wait_send()
        for u in range(n_units):
            for cp in (d_x(u), d_xd(u) if kind(u) == "x" else d_dg(u), d_y(u), d_z(u), d_s(u, q_own, 4),
                       d_s(u, q_y, 5), d_s(u, q_z, 6), d_s(u, q_d, 7)):
                cp.wait_send()

    def d_bias(i):
        dev = [sib, xn, m_sx][i]
        return rc(bias, biasg.at[mp], b_s.at[i], b_r.at[i], (dp, dev))

    for u in range(3):
        d_x(u).start()
    d_own(0).start()
    c_own(0).start()
    for i in range(3):
        d_bias(i).start()
    for u in range(3):
        d_xd(u).start()
    for u in range(3, n_units):
        d_x(u).start()
        if kind(u) == "x":
            d_xd(u).start()
    for t in range(1, 4):
        d_own(t).start()
        if t < 3:
            c_own(t).start()

    def rows_of(ref, r0, n):
        return ref.at[pl.ds(pl.multiple_of(r0, 16), n), :]

    half = CHUNK // 2

    def d_xs(t):
        return rc(rows_of(xsend, t * CHUNK, CHUNK), rows_of(xrecv, t * CHUNK, CHUNK), x_s.at[t], x_r.at[t], dev_x)

    def d_ys(t):
        return rc(rows_of(keep, t * CHUNK + (1 - y) * half, half), rows_of(yrecv, t * half, half),
                  y_s.at[t], y_r.at[t], dev_y)

    def piece_at(t, zj):
        return t * CHUNK + y * half + zj * piece

    def d_zs(t, o):
        j = t * (nz - 1) + o - 1
        return rc(rows_of(keep, piece_at(t, (zi + o) % nz), piece), rows_of(zrecv, j * piece, piece),
                  z_s.at[j], z_r.at[j], (z_devs[o - 1], mp))

    def d_as(t, o):
        j = t * (nz - 1) + o - 1
        return rc(rows_of(fin, t * piece, piece), rows_of(gsum, piece_at(t, zi), piece),
                  a_s.at[j], a_r.at[j], (z_devs[o - 1], mp))

    def d_ar(t, o):
        j = t * (nz - 1) + o - 1
        r = rows_of(gsum, piece_at(t, (zi + nz - o) % nz), piece)
        return rc(r, r, a_s.at[j], a_r.at[j], (z_devs[o - 1], mp))

    def d_os(t, o):
        j = t * (n_out - 1) + o - 1
        return rc(rows_of(fin, t * piece, piece), rows_of(orecv, j * piece, piece),
                  o_s.at[j], o_r.at[j], (o_devs[o - 1], mp))

    def c_ls(t):
        return pltpu.make_async_copy(rows_of(fin, t * piece, piece), rows_of(gsum, piece_at(t, zi), piece), l_s.at[t])

    def d_es(t):
        r = rows_of(gsum, t * CHUNK + y * half, half)
        return rc(r, r, e_s.at[t], e_r.at[t], dev_y)

    def d_er(t):
        r = rows_of(gsum, t * CHUNK + (1 - y) * half, half)
        return rc(r, r, e_s.at[t], e_r.at[t], dev_y)

    def get(ref, r0, n):
        return ref[pl.ds(pl.multiple_of(r0, 16), n), :].astype(F32)

    def put(ref, r0, n, val):
        ref[pl.ds(pl.multiple_of(r0, 16), n), :] = val.astype(BF16)

    def st_y(t):
        d_xs(t).wait_recv()
        r0 = t * CHUNK
        put(keep, r0, CHUNK, get(keep, r0, CHUNK) + get(xrecv, r0, CHUNK))
        d_ys(t).start()

    def st_z(t):
        d_ys(t).wait_recv()
        r0 = t * CHUNK + y * half
        put(keep, r0, half, get(keep, r0, half) + get(yrecv, t * half, half))
        for o in range(1, nz):
            d_zs(t, o).start()

    def st_a(t):
        for o in range(1, nz):
            d_zs(t, o).wait_recv()
        acc = get(keep, piece_at(t, zi), piece)
        for o in range(1, nz):
            acc = acc + get(zrecv, (t * (nz - 1) + o - 1) * piece, piece)
        put(fin, t * piece, piece, acc)
        if n_out == 1:
            st_g(t)
        else:
            for o in range(1, n_out):
                d_os(t, o).start()

    def st_o(t):
        own_part = get(fin, t * piece, piece)
        acc = own_part
        for o in range(1, n_out):
            d_os(t, o).wait_recv()
            d_os(t, o).wait_send()
        me = dp // inner
        acc = jnp.zeros_like(own_part)
        for gidx in range(n_out):
            slot = (me - gidx + n_out) % n_out
            r0 = (t * (n_out - 1) + jnp.maximum(slot, 1) - 1) * piece
            acc = acc + jnp.where(slot == 0, own_part, get(orecv, r0, piece))
        put(fin, t * piece, piece, acc)
        st_g(t)

    def st_g(t):
        c_ls(t).start()
        for o in range(1, nz):
            d_as(t, o).start()

    def st_b(t):
        c_ls(t).wait()
        for o in range(1, nz):
            d_ar(t, o).wait_recv()
        d_es(t).start()

    def st_e(t):
        d_er(t).wait_recv()
        d_xs(t).wait_send()
        d_ys(t).wait_send()
        d_es(t).wait_send()
        for o in range(1, nz):
            d_zs(t, o).wait_send()
            d_as(t, o).wait_send()

    stages = [st_y, st_z, st_a] + ([st_o] if n_out > 1 else []) + [st_b, st_e]

    gap = 2

    def tick(t):
        for s in reversed(range(len(stages))):
            u = t - gap * s

            @pl.when(jnp.logical_and(u >= 0, u < n_chunks))
            def _(s=s, u=u):
                stages[s](u)

    def d_c(slot, r0, n, j):
        part = pl.ds(pl.multiple_of(r0, 16), n)
        return rc(csend.at[slot, part, :], crecv.at[slot, part, :], c_s.at[slot, j], c_r.at[slot, j], dev_s)

    def m_of(i):
        mx = jnp.where(i < 2, 1 - x, x)
        mc = jnp.where(i % 2 == 0, 1 - c, c)
        return 2 * mx + mc

    small[...] = jnp.zeros_like(small)
    rb = 128

    def ln1(i):
        r = pl.ds(pl.multiple_of(i * rb, rb), rb)
        xv = tok[r, :].astype(F32)
        xc = xv - jnp.mean(xv, axis=-1, keepdims=True)
        inv = lax.rsqrt(jnp.mean(xc * xc, axis=-1, keepdims=True) + EPS)
        n1[r, :] = (xc * inv * g1[...] + s1[...]).astype(BF16)

    c_tok.wait()
    loop(rows // rb, ln1)

    n_seg = lens.shape[1]
    col = lax.broadcasted_iota(jnp.int32, (rows, 1), 0)
    row = lax.broadcasted_iota(jnp.int32, (1, rows), 1)
    seg_col, seg_row = jnp.zeros_like(col), jnp.zeros_like(row)
    bound = jnp.int32(0)
    for j in range(n_seg):
        bound = bound + lens[mp, j]
        seg_col = seg_col + (col >= bound).astype(jnp.int32)
        seg_row = seg_row + (row >= bound).astype(jnp.int32)
    mask[...] = jnp.where(seg_col == seg_row, 0.0, -1000000000.0).astype(F32)
    kept = (seg_col < n_seg - 1).astype(F32)

    biasg[mp] = bias[...]
    for i in range(3):
        d_bias(i).wait()
    tot = biasg[0]
    for m in range(1, 4):
        tot = tot + pltpu.roll(biasg[m], hw * m, 1)
    qvb[...] = tot
    do((1, 0))

    scale = 1.0 / math.sqrt(HD)
    n_pairs = d // (2 * HD)
    per_half = n_pairs // 2
    low_half = lax.broadcasted_iota(jnp.int32, (1, 2 * HD), 1) < HD
    ab = rows // 2

    def lanes_of(i):
        xh = jnp.where(i < per_half, x, 1 - x)
        pair = xh * per_half + i % per_half
        return xh, pair, pl.ds(pl.multiple_of(pair * 2 * HD, 128), 2 * HD)

    def pick(h, val):
        zero = jnp.zeros_like(val)
        return jnp.where(low_half, val, zero) if h == 0 else jnp.where(low_half, zero, val)

    def attn_fwd(i):
        xh, pair, lanes = lanes_of(i)

        @pl.when(i == 0)
        def _():
            near(0)

        @pl.when(i == per_half)
        def _():
            far(0)

        @pl.when(i % per_half == 0)
        def _():
            w_rows = pl.ds(pl.multiple_of(xh * half_w, 128), half_w)
            w_lanes = w_rows
            for cc, ref in enumerate((q, k, v)):
                val = nt(n1[...], wq[cc, w_rows, :])
                if cc == 0:
                    val = val + qvb[1:2, w_lanes]
                if cc == 2:
                    val = val + qvb[2:3, w_lanes]
                val = val.astype(BF16)
                if cc == 0:
                    val = val * jnp.asarray(scale, BF16)
                ref[:, w_lanes] = val

        k2, v2 = k[:, lanes], v[:, lanes]
        for r in range(2):
            rs = pl.ds(r * ab, ab)
            q2 = q[rs, lanes]
            outs = []
            for h in range(2):
                sc = nt(pick(h, q2), k2) + mask[rs, :]
                e = jnp.exp(sc - jnp.max(sc, axis=-1, keepdims=True))
                pr = (e * (1.0 / jnp.sum(e, axis=-1, keepdims=True))).astype(BF16)
                p[2 * pair + h, rs, :] = pr
                outs.append(nn(pr, v2))
            o2 = jnp.where(low_half, outs[0], outs[1]) * kept[r * ab:(r + 1) * ab]
            att[rs, lanes] = o2.astype(BF16)

            for at, todo in AG_PLAN.items():
                if at % 2 == r:
                    @pl.when(i == at // 2)
                    def _(todo=todo):
                        do(*todo)

    AG_PLAN = {
        0: [(1, 1), (1, 2)],
        1: [(2, 0)],
        2: [(2, 1), (3, 0)],
        4: [(2, 2), (3, 1)],
        5: [(3, 2)],
        6: [(1, 3), (3, 3), (2, 3)],
        7: [(1, 4)],
        8: [(1, 5)],
        9: [(2, 4)],
        10: [(1, 6)],
        11: [(1, 7), (2, 5)],
    }
    loop(n_pairs, attn_fwd)

    near(1)
    far(1)
    mixed[...] = nn(att[...], wo[...])
    do((1, 8), (2, 6), (3, 4))

    def ln2(i):
        r = pl.ds(pl.multiple_of(i * rb, rb), rb)
        xv = tok[r, :].astype(F32) + mixed[r, :] + ob[...]
        mixed[r, :] = xv
        lo[r, :] = xv + db[...]
        xc = xv - jnp.mean(xv, axis=-1, keepdims=True)
        inv = lax.rsqrt(jnp.mean(xc * xc, axis=-1, keepdims=True) + EPS)
        n2[r, :] = (xc * inv * g2[...] + s2[...]).astype(BF16)

    loop(rows // rb, ln2)
    do((2, 7), (3, 5), (1, 9), (3, 6), (1, 10), (3, 7))

    tile = 256

    def emit_block(g, i, make):
        slot, mine = i // 2, i % 2 == 1
        n_parts = d // tile
        if g > 0:
            @pl.when(jnp.logical_not(mine))
            def _():
                pl.semaphore_wait(credit.at[slot], 1)
                for r in range(n_parts):
                    d_c(slot, r * tile, tile, r).wait_send()

        def part(r):
            rr = pl.ds(pl.multiple_of(r * tile, tile), tile)
            res = make(r)

            @pl.when(jnp.logical_not(mine))
            def _():
                csend[slot, rr, :] = res.astype(BF16)
                d_c(slot, r * tile, tile, r).start()

            @pl.when(mine)
            def _():
                d_c(slot, r * tile, tile, r).wait_recv()
                tot = (res + crecv[slot, rr, :].astype(F32)).astype(BF16)
                out = pl.ds(pl.multiple_of(g * d + r * tile, tile), tile)

                @pl.when(slot == 0)
                def _():
                    xsend[out, :] = tot
                    for cc in range(tile // CHUNK):
                        d_xs(g * per_group + r * (tile // CHUNK) + cc).start()

                @pl.when(slot == 1)
                def _():
                    keep[out, :] = tot

        loop(n_parts, part)

        @pl.when(mine)
        def _():
            pl.semaphore_signal(credit.at[slot], inc=1, device_id=dev_s, device_id_type=MESH)

    near(2)
    far(2)

    c_cot.wait()

    def ffn1(i):
        m = m_of(i)

        def hid(n):
            nl = pl.ds(pl.multiple_of(n * tile, tile), tile)
            h = nn(n2[...], wu[m, :, nl]) + biasg[m, 0:1, nl]
            phi = 0.5 * (1.0 + lax.erf(h * INV_SQRT2))
            act[m, :, nl] = (h * phi).astype(BF16)
            gp[m, :, nl] = (phi + h * jnp.exp(-0.5 * h * h) * INV_SQRT2PI).astype(BF16)

        loop(ff // tile, hid)

        def make(r):
            rl = pl.ds(pl.multiple_of(r * tile, tile), tile)
            return tn(act[m, :, rl], cot[...])

        emit_block(0, i, make)

        for at, todo in enumerate(([(1, 11), (2, 8), (2, 9), (3, 8)], [(2, 10), (3, 9), (2, 11)], [(3, 10), (3, 11)])):
            @pl.when(i == at)
            def _(todo=todo):
                do(*todo)

    loop(4, ffn1)

    near(3)
    far(3)

    def c_wd(i):
        return pltpu.make_async_copy(wd_full.at[m_of(i)], wdbuf.at[i % 2], wd_sem.at[i % 2])

    def start_wd(i):
        @pl.when(i < 3)
        def _():
            c_wd(i).start()

        @pl.when(i == 3)
        def _():
            pltpu.make_async_copy(wd_in, wdbuf.at[i % 2], wd_sem.at[i % 2]).start()

    start_wd(0)
    mg[...] = jnp.zeros_like(mg)

    def ffn2(i):
        m = m_of(i)
        c_wd(i).wait()

        @pl.when(i < 3)
        def _():
            start_wd(i + 1)

        s = i % 2

        def hg(n):
            nl = pl.ds(pl.multiple_of(n * tile, tile), tile)
            val = (gp[m, :, nl].astype(F32) * nt(cot[...], wdbuf[s, nl, :])).astype(BF16)
            gp[m, :, nl] = val
            small[pl.ds(8 + m, 1), nl] = jnp.sum(val.astype(F32), axis=0, keepdims=True)

        loop(ff // tile, hg)

        def make(r):
            rl = pl.ds(pl.multiple_of(r * tile, tile), tile)
            return tn(n2[:, rl], gp[m])

        emit_block(1, i, make)
        tick(jnp.where(i == 0, 0, i + 1))

        def back(n):
            nl = pl.ds(pl.multiple_of(n * tile, tile), tile)
            mg[:, nl] += nt(gp[m], wu[m, nl, :])
            lo[:, nl] += nn(act[m], wdbuf[s, :, nl])

        loop(d // tile, back)

        @pl.when(i == 0)
        def _():
            tick(1)

    loop(4, ffn2)
    c_lo.start()

    def ln2b(i):
        r = pl.ds(pl.multiple_of(i * rb, rb), rb)
        xv = mixed[r, :]
        xc = xv - jnp.mean(xv, axis=-1, keepdims=True)
        inv = lax.rsqrt(jnp.mean(xc * xc, axis=-1, keepdims=True) + EPS)
        xh = xc * inv
        dn = mg[r, :]
        small[2:3, :] += jnp.sum(dn * xh, axis=0, keepdims=True)
        small[3:4, :] += jnp.sum(dn, axis=0, keepdims=True)
        gg = dn * g2[...]
        val = cot[r, :].astype(F32) + (
            gg - jnp.mean(gg, axis=-1, keepdims=True) - xh * jnp.mean(gg * xh, axis=-1, keepdims=True)
        ) * inv
        mg[r, :] = val
        mgl[r, :] = val.astype(BF16)
        small[4:5, :] += jnp.sum(val, axis=0, keepdims=True)
        small[5:6, :] += jnp.sum(cot[r, :].astype(F32), axis=0, keepdims=True)

    loop(rows // rb, ln2b)

    da = n2

    def dab(n):
        nl = pl.ds(pl.multiple_of(n * tile, tile), tile)
        da[:, nl] = (nt(mgl[...], wo[nl, :]).astype(BF16).astype(F32) * kept).astype(BF16)

    loop(d // tile, dab)
    tick(5)

    def attn_bwd(i):
        xh, pair, lanes = lanes_of((i + per_half) % n_pairs)
        k2, v2 = k[:, lanes], v[:, lanes]
        do2, q2 = da[:, lanes], q[:, lanes]
        dqs, dks, dvs = [], [], []
        for h in range(2):
            dq_rows = []
            for r in range(2):
                rs = slice(r * ab, (r + 1) * ab)
                dpv = nt(pick(h, do2[rs]), v2)
                pr = p[2 * pair + h, pl.ds(r * ab, ab), :].astype(F32)
                t1 = pr * dpv
                ds = (t1 - pr * jnp.sum(t1, axis=-1, keepdims=True)).astype(BF16)
                dsb[pl.ds(r * ab, ab), :] = ds
                dq_rows.append(nn(ds, k2))
            dqs.append(jnp.concatenate(dq_rows, axis=0))
            dks.append(tn(dsb[...], q2))
            dvs.append(tn(p[2 * pair + h], do2))
        dv2 = jnp.where(low_half, dvs[0], dvs[1]).astype(BF16)
        dk2 = jnp.where(low_half, dks[0], dks[1]).astype(BF16)
        dq2 = (jnp.where(low_half, dqs[0], dqs[1]) * scale).astype(BF16)
        q[:, lanes] = dq2
        k[:, lanes] = dk2
        v[:, lanes] = dv2
        small[6:7, lanes] = jnp.sum(dq2.astype(F32), axis=0, keepdims=True)
        small[7:8, lanes] = jnp.sum(dv2.astype(F32), axis=0, keepdims=True)

        @pl.when(i % per_half == per_half - 1)
        def _():
            a = i // per_half
            wl = pl.ds(pl.multiple_of(xh * half_w, 128), half_w)
            pl.semaphore_wait(credit.at[a], 1)
            for r in range(d // tile):
                d_c(a, r * tile, tile, r).wait_send()
            for j, (ref, other) in enumerate(((att, mgl), (q, n1), (k, n1), (v, n1))):
                act[pl.ds(0, 2), pl.ds(0, hw), :] = tn(ref[:, wl], other[...]).astype(BF16).reshape(2, hw, d)
                csend[a, j * hw:(j + 1) * hw, :] = act[1 - c, 0:hw, :]
                d_c(a, j * hw, hw, j).start()
                gp[0 if j < 2 else 1, (j % 2) * hw:(j % 2 + 1) * hw, :] = act[c, 0:hw, :]
            for j in range(4):
                d_c(a, j * hw, hw, j).wait_recv()
                tot = (gp[0 if j < 2 else 1, (j % 2) * hw:(j % 2 + 1) * hw, :].astype(F32)
                       + crecv[a, j * hw:(j + 1) * hw, :].astype(F32)).astype(BF16)

                @pl.when(a == 0)
                def _():
                    xsend[2 * d + j * hw:2 * d + (j + 1) * hw, :] = tot

                @pl.when(a == 1)
                def _():
                    keep[2 * d + j * hw:2 * d + (j + 1) * hw, :] = tot

            @pl.when(a == 0)
            def _():
                for cc in range(per_group):
                    d_xs(2 * per_group + cc).start()

        tick(6 + i)

    loop(n_pairs, attn_bwd)

    def ln1n(n):
        nl = pl.ds(pl.multiple_of(n * tile, tile), tile)
        tg[:, nl] = nn(q[...], wq[0, :, nl]) + nn(k[...], wq[1, :, nl]) + nn(v[...], wq[2, :, nl])

    loop(d // tile, ln1n)

    def ln1b(i):
        r = pl.ds(pl.multiple_of(i * rb, rb), rb)
        xv = tok[r, :].astype(F32)
        xc = xv - jnp.mean(xv, axis=-1, keepdims=True)
        inv = lax.rsqrt(jnp.mean(xc * xc, axis=-1, keepdims=True) + EPS)
        xh = xc * inv
        dn = tg[r, :]
        small[0:1, :] += jnp.sum(dn * xh, axis=0, keepdims=True)
        small[1:2, :] += jnp.sum(dn, axis=0, keepdims=True)
        gg = dn * g1[...]
        tg[r, :] = mg[r, :] + (
            gg - jnp.mean(gg, axis=-1, keepdims=True) - xh * jnp.mean(gg * xh, axis=-1, keepdims=True)
        ) * inv

    loop(rows // rb, ln1b)
    c_tg.start()

    v_devs = [(dp, sib), (dp, xn)] + [(flip(dp, b), mp) for b in bits]

    def d_v(s):
        return rc(small, srecv.at[s], v_s.at[s], v_r.at[s], v_devs[s])

    first = 6 + n_pairs

    def tail(i):
        for s in range(len(v_devs) + 1):
            @pl.when(i == s)
            def _(s=s):
                if s > 0:
                    d_v(s - 1).wait()
                    small[...] += srecv[s - 1]
                if s < len(v_devs):
                    d_v(s).start()

        tick(first + i)

    loop(max(n_chunks + gap * (len(stages) - 1) - first, len(v_devs) + 1), tail)
    for slot in range(2):
        for j in range(4):
            d_c(slot, j * hw, hw, j).wait_send()
    sent()
    c_lo.wait()
    c_tg.wait()


def layer(n_dp, tokens, lens, g1, s1, wqkv, qvb, wo, ob, g2, s2, wu, ub, wd, db, cot):
    rows, d = tokens.shape
    hw, ff = wo.shape[0], wu.shape[1]
    n_mp = lax.axis_size("mp")
    mp = lax.axis_index("mp")
    inner = min(n_dp, 8)
    nz, n_out = inner // 2, n_dp // inner
    piece = CHUNK // 2 // nz
    nc = 3 * d // CHUNK
    n_small = 2 + n_dp.bit_length() - 1
    heads = d // HD
    wqt = jnp.swapaxes(wqkv, 1, 2)
    vm = pl.BlockSpec(memory_space=pltpu.VMEM)
    hbm = pl.BlockSpec(memory_space=pl.ANY)
    sm = pl.BlockSpec(memory_space=pltpu.SMEM)
    dma = pltpu.SemaphoreType.DMA
    S = jax.ShapeDtypeStruct
    V = pltpu.VMEM
    nzr = max(nc * (nz - 1), 1)
    nor = max(nc * (n_out - 1), 1)
    lo, tg, gsum, small, _ = pl.pallas_call(
        functools.partial(body, n_dp),
        out_shape=(
            S((rows, d), F32), S((rows, d), F32), S((3 * d, d), BF16), S((16, d), F32), S((n_mp, ff, d), BF16),
        ),
        in_specs=[sm] + [hbm] * 2 + [vm] * 8 + [hbm] * 4,
        out_specs=(hbm, hbm, hbm, vm, hbm),
        scratch_shapes=[
            V((rows, d), BF16), V((rows, d), BF16), V((rows, d), F32), V((rows, d), F32), V((8, d), F32), V((8, d), F32),
            V((8, d), F32),
            V((3, d, d), BF16), V((d, d), BF16), V((n_mp, d, ff), BF16), V((2, ff, d), BF16), V((n_mp, 8, d), F32),
            V((rows, d), BF16), V((rows, d), BF16), V((rows, d), BF16), V((rows, d), BF16),
            V((heads, rows, rows), BF16), V((rows, rows), BF16), V((rows, d), BF16),
            V((rows, d), F32), V((rows, d), F32), V((rows, d), BF16), V((rows, d), BF16),
            V((n_mp, rows, ff), BF16), V((n_mp, rows, ff), BF16), V((rows, rows), F32),
            V((2, d, d), BF16), V((2, d, d), BF16), V((3 * d, d), BF16), V((3 * d, d), BF16), V((3 * d, d), BF16),
            V((nc * CHUNK // 2, d), BF16), V((nzr * piece, d), BF16), V((nc * piece, d), BF16),
            V((nor * piece, d), BF16), V((n_small, 16, d), F32),
            dma((4,)), dma((4,)), dma((4,)), dma((4,)), dma((4,)), dma((12, 8)), dma((12, 4)), dma((3,)), dma((3,)),
            dma((2,)), dma((2, 4)), dma((2, 4)),
            pltpu.SemaphoreType.REGULAR((2,)), dma((nc,)), dma((nc,)), dma((nc,)), dma((nc,)),
            dma((nzr,)), dma((nzr,)), dma((nzr,)), dma((nzr,)), dma((nc,)), dma((nc,)), dma((nc,)),
            dma((nor,)), dma((nor,)), dma((n_small,)), dma((n_small,)),
        ],
        compiler_params=pltpu.CompilerParams(
            collective_id=0, has_side_effects=True, vmem_limit_bytes=67043328
        ),
        name="layer",
    )(lens, tokens, cot, g1, s1, ob, g2, s2, db, ub, qvb, wqt, wo, wu, wd)

    steps = 8
    part, rpart = d // steps, rows // steps
    opart = hw // 2

    def finish(down, up, rest, lo_ref, tg_ref, sm_ref, o_down, o_up, o_out, o_qkv, o_lo, o_tg,
               o_g1, o_s1, o_g2, o_s2, o_ob, o_db, o_qv, o_ub):
        i = pl.program_id(0)
        o_down[...] = down[...].astype(F32)
        o_up[...] = up[...].astype(F32)
        o_lo[...] = lo_ref[...]
        o_tg[...] = tg_ref[...]

        @pl.when(i < 2)
        def _():
            o_out[...] = rest[...].astype(F32)

        @pl.when(i >= 2)
        def _():
            o_qkv[0] = rest[...].astype(F32)

        @pl.when(i == 0)
        def _():
            for n, ref in enumerate((o_g1, o_s1, o_g2, o_s2, o_ob, o_db)):
                ref[...] = sm_ref[n:n + 1, :].reshape(d)
            me = lax.axis_index("mp")
            o_ub[...] = sm_ref[pl.ds(8 + me, 1), :].reshape(d)
            acc = jnp.zeros((2, hw), F32)
            for m in range(n_mp):
                acc = jnp.where(me == m, sm_ref[6:8, m * hw:(m + 1) * hw], acc)
            o_qv[...] = acc

    blk = lambda off: pl.BlockSpec((part, d), lambda i: (i + off, 0))
    row = pl.BlockSpec((rpart, d), lambda i: (i, 0))
    one = pl.BlockSpec((d,), lambda i: (0,))
    dwn, up_g, out_g, qkv_g, lo, tg, o_g1, o_s1, o_g2, o_s2, o_ob, o_db, o_qv, o_ub = pl.pallas_call(
        finish,
        grid=(steps,),
        out_shape=(
            S((ff, d), F32), S((d, ff), F32), S((hw, d), F32), S((3, hw, d), F32), S((rows, d), F32), S((rows, d), F32),
            S((d,), F32), S((d,), F32), S((d,), F32), S((d,), F32), S((d,), F32), S((d,), F32), S((2, hw), F32), S((d,), F32),
        ),
        in_specs=[blk(0), blk(steps), blk(2 * steps), row, row, pl.BlockSpec((16, d), lambda i: (0, 0))],
        out_specs=(
            blk(0), blk(0), pl.BlockSpec((opart, d), lambda i: (jnp.minimum(i, 1), 0)),
            pl.BlockSpec((1, opart, d), lambda i: (jnp.maximum(i - 2, 0) // 2, jnp.maximum(i - 2, 0) % 2, 0)), row, row,
            one, one, one, one, one, one, pl.BlockSpec((2, hw), lambda i: (0, 0)), one,
        ),
        name="finish",
    )(gsum, gsum, gsum, lo, tg, small)
    return (
        lo, tg, o_g1, o_s1, jnp.swapaxes(qkv_g, 1, 2), o_qv, out_g, o_ob, o_g2, o_s2, up_g, o_ub, dwn, o_db,
    )


def solution(mesh):
    rows = P(("dp", "mp"), None)
    in_specs = (
        rows, P("dp", None), P(), P(), P(None, None, "mp"), P(None, "mp"), P("mp", None), P(), P(), P(),
        P(None, "mp"), P("mp"), P("mp", None), P(), rows,
    )
    out_specs = (
        rows, rows, P(), P(), P(None, None, "mp"), P(None, "mp"), P("mp", None), P(), P(), P(),
        P(None, "mp"), P("mp"), P("mp", None), P(),
    )
    return jax.shard_map(
        functools.partial(layer, mesh.shape["dp"]), mesh=mesh, in_specs=in_specs, out_specs=out_specs, check_vma=False
    )
```

```python
import functools
import math

import jax
import jax.numpy as jnp
from jax import lax
from jax.experimental import pallas as pl
from jax.experimental.pallas import tpu as pltpu
from jax.sharding import PartitionSpec as P

MESH = pl.DeviceIdType.MESH
F32, BF16 = jnp.float32, jnp.bfloat16
HD = 64
EPS = 1e-05
CHUNK = 128
INV_SQRT2 = 1.0 / math.sqrt(2.0)
INV_SQRT2PI = 1.0 / math.sqrt(2.0 * math.pi)


def dot(a, b, dims):
    return lax.dot_general(a, b, (dims, ((), ())), preferred_element_type=F32)


def nn(a, b):
    return dot(a, b, ((1,), (0,)))


def nt(a, b):
    return dot(a, b, ((1,), (1,)))


def tn(a, b):
    return dot(a, b, ((0,), (0,)))


def loop(n, fn):
    lax.fori_loop(0, n, lambda i, c: (fn(i), c)[1], 0)


def flip(value, bit):
    return value + bit * (1 - 2 * ((value // bit) % 2))


def body(
    n_dp,
    lens, tok_in, cot_in, g1, s1, ob, g2, s2, db, ub_in, qvb_in, wq_in, wo_in, wu_in, wd_in,
    lo_out, tg_out, gsum, small, wd_full,
    tok, cot, lo, tg, bias, vecs, qvb,
    wq, wo, wu, wdbuf, biasg, n1, q, k, v, p, dsb, att, mixed, mg, n2, mgl, act, gp, mask,
    csend, crecv, xsend, keep, xrecv, yrecv, zrecv, fin, orecv, srecv,
    io_sem, own_sem, own_s, own_r, far_r, ag_s, ag_r, b_s, b_r, wd_sem, c_s, c_r, credit, x_s, x_r, y_s, y_r, z_s, z_r,
    a_s, a_r, e_s, e_r, l_s, o_s, o_r, v_s, v_r,
):
    rows, d = tok.shape
    c_tok = pltpu.make_async_copy(tok_in, tok, io_sem.at[0])
    c_cot = pltpu.make_async_copy(cot_in, cot, io_sem.at[1])
    c_lo = pltpu.make_async_copy(lo, lo_out, io_sem.at[2])
    c_tg = pltpu.make_async_copy(tg, tg_out, io_sem.at[3])
    c_tok.start()
    c_cot.start()
    hw = wo_in.shape[0]
    ff = wu_in.shape[1]
    half_w = 2 * hw
    dp, mp = lax.axis_index("dp"), lax.axis_index("mp")
    x, c = mp // 2, mp % 2
    y, zz = dp % 2, dp // 2
    inner = min(n_dp, 8)
    nz = inner // 2
    n_out = n_dp // inner
    z1, zi, base = zz % 2, zz % nz, dp - dp % inner
    sib, xn = flip(mp, 1), flip(mp, 2)
    yn, zn = flip(dp, 1), flip(dp, 2)
    m_x, m_sx = xn, flip(xn, 1)
    groups = 3
    piece = CHUNK // 2 // nz
    per_group = d // CHUNK
    n_chunks = groups * per_group

    def rc(src, dst, ss, rs, dev):
        return pltpu.make_async_remote_copy(
            src_ref=src, dst_ref=dst, send_sem=ss, recv_sem=rs, device_id=dev, device_id_type=MESH
        )

    z_devs = [base + 2 * ((zi + o) % nz) + y for o in range(1, nz)]
    o_devs = [(dp + inner * o) % n_dp for o in range(1, n_out)]
    bits = [1 << b for b in range(n_dp.bit_length() - 1)]
    peers_dp = [yn] + z_devs + o_devs
    peers = [(dp, sib), (dp, xn), (dp, m_sx)] + [(e, mp) for e in peers_dp]

    bias[...] = jnp.zeros_like(bias)
    bias[0:1, :] = ub_in[...].reshape(1, d)
    bias[1:3, 0:hw] = qvb_in[...]
    for n, ref in enumerate((g1, s1, ob, g2, s2, db)):
        vecs[n:n + 1, :] = ref[...].reshape(1, d)
    g1, s1, ob, g2, s2, db = (vecs.at[pl.ds(n, 1)] for n in range(6))
    barrier = pltpu.get_barrier_semaphore()
    for dev in peers:
        pl.semaphore_signal(barrier, inc=1, device_id=dev, device_id_type=MESH)
    pl.semaphore_wait(barrier, len(peers))

    n_units = 12
    quarter = hw // 4

    def own(u, r0, n):
        if u < 3:
            return wq_in.at[u, pl.ds(r0, n), :]
        if u == 3:
            return wo_in.at[pl.ds(r0, n), :]
        return (wu_in if u < 8 else wd_in).at[pl.ds((u % 4) * hw + r0, n), :]

    def full(u, m, r0, n):
        if u < 4:
            return (wq.at[u] if u < 3 else wo).at[pl.ds(pl.multiple_of(m * hw + r0, 16), n), :]
        return (wu if u < 8 else wd_full).at[m, pl.ds((u % 4) * hw + r0, n), :]

    q_own = y + 2 * z1
    q_y, q_z, q_d = (1 - y) + 2 * z1, y + 2 * (1 - z1), (1 - y) + 2 * (1 - z1)

    def start_of(qq):
        return pl.multiple_of(qq * quarter, 16)

    def reg(u, m, qq):
        return full(u, m, start_of(qq), quarter)

    def shard_in(t):
        return (wq_in, wo_in, wu_in, wd_in)[t]

    def whole(t, m):
        if t == 0:
            return wq.at[:, pl.ds(pl.multiple_of(m * hw, 16), hw), :]
        if t == 1:
            return wo.at[pl.ds(pl.multiple_of(m * hw, 16), hw), :]
        return (wu, wd_full)[t - 2].at[m]

    def tensor_of(u):
        return 0 if u < 3 else 1 if u == 3 else 2 if u < 8 else 3

    def kind(u):
        return "xyz"[u % 3]

    dev_s, dev_x, dev_y, dev_z = (dp, sib), (dp, xn), (yn, mp), (zn, mp)

    def c_own(t):
        return pltpu.make_async_copy(shard_in(t), whole(t, mp), own_sem.at[t])

    def d_own(t):
        return rc(shard_in(t), whole(t, mp), own_s.at[t], own_r.at[t], dev_s)

    def d_x(u):
        return rc(own(u, start_of(q_own), quarter), reg(u, mp, q_own), ag_s.at[u, 0], ag_r.at[u, 0], dev_x)

    def d_xd(u):
        return rc(own(u, start_of(q_d), quarter), reg(u, mp, q_d), ag_s.at[u, 1], ag_r.at[u, 1], dev_x)

    def fwd(u, qq, si, rs, dev):
        r = reg(u, m_x, qq)
        return rc(r, r, ag_s.at[u, si], rs, dev)

    def d_y(u):
        return fwd(u, q_own, 2, ag_r.at[u, 2], dev_y)

    def d_z(u):
        return fwd(u, q_own, 3, ag_r.at[u, 3], dev_z)

    def d_s(u, qq, si):
        return fwd(u, qq, si, far_r.at[tensor_of(u)], dev_s)

    def d_dg(u):
        if kind(u) == "y":
            return fwd(u, q_z, 1, ag_r.at[u, 1], dev_y)
        return fwd(u, q_y, 1, ag_r.at[u, 1], dev_z)

    def arrive(region, sem, dev):
        rc(region, region, ag_s.at[0, 0], sem, dev).wait_recv()

    def f1(u):
        arrive(reg(u, m_x, q_own), ag_r.at[u, 0], dev_x)
        d_y(u).start()
        d_z(u).start()
        d_s(u, q_own, 4).start()

    def f2(u):
        arrive(reg(u, m_x, q_y), ag_r.at[u, 2], dev_y)
        arrive(reg(u, m_x, q_z), ag_r.at[u, 3], dev_z)
        if kind(u) != "x":
            d_dg(u).start()
        d_s(u, q_y, 5).start()
        d_s(u, q_z, 6).start()

    def f3(u):
        arrive(reg(u, m_x, q_d), ag_r.at[u, 1], {"x": dev_x, "y": dev_y, "z": dev_z}[kind(u)])
        d_s(u, q_d, 7).start()

    def do(*todo):
        for step, u in todo:
            (f1, f2, f3)[step - 1](u)

    def near(t):
        if t < 3:
            c_own(t).wait()
        arrive(whole(t, sib), own_r.at[t], dev_s)

    def far(t):
        arrive(whole(t, m_sx), far_r.at[t], dev_s)

    def sent():
        for t in range(4):
            d_own(t).wait_send()
        for u in range(n_units):
            for cp in (d_x(u), d_xd(u) if kind(u) == "x" else d_dg(u), d_y(u), d_z(u), d_s(u, q_own, 4),
                       d_s(u, q_y, 5), d_s(u, q_z, 6), d_s(u, q_d, 7)):
                cp.wait_send()

    def d_bias(i):
        dev = [sib, xn, m_sx][i]
        return rc(bias, biasg.at[mp], b_s.at[i], b_r.at[i], (dp, dev))

    for u in range(3):
        d_x(u).start()
    d_own(0).start()
    c_own(0).start()
    for i in range(3):
        d_bias(i).start()
    d_xd(0).start()
    for u in range(3, n_units):
        d_x(u).start()
        if u % 3 == 2:
            d_xd(u - 2).start()
    for t in range(1, 4):
        d_own(t).start()
        if t < 3:
            c_own(t).start()

    def rows_of(ref, r0, n):
        return ref.at[pl.ds(pl.multiple_of(r0, 16), n), :]

    half = CHUNK // 2

    def d_xs(t):
        return rc(rows_of(xsend, t * CHUNK, CHUNK), rows_of(xrecv, t * CHUNK, CHUNK), x_s.at[t], x_r.at[t], dev_x)

    def d_ys(t):
        return rc(rows_of(keep, t * CHUNK + (1 - y) * half, half), rows_of(yrecv, t * half, half),
                  y_s.at[t], y_r.at[t], dev_y)

    def piece_at(t, zj):
        return t * CHUNK + y * half + zj * piece

    def d_zs(t, o):
        j = t * (nz - 1) + o - 1
        return rc(rows_of(keep, piece_at(t, (zi + o) % nz), piece), rows_of(zrecv, j * piece, piece),
                  z_s.at[j], z_r.at[j], (z_devs[o - 1], mp))

    def d_as(t, o):
        j = t * (nz - 1) + o - 1
        return rc(rows_of(fin, t * piece, piece), rows_of(gsum, piece_at(t, zi), piece),
                  a_s.at[j], a_r.at[j], (z_devs[o - 1], mp))

    def d_ar(t, o):
        j = t * (nz - 1) + o - 1
        r = rows_of(gsum, piece_at(t, (zi + nz - o) % nz), piece)
        return rc(r, r, a_s.at[j], a_r.at[j], (z_devs[o - 1], mp))

    def d_os(t, o):
        j = t * (n_out - 1) + o - 1
        return rc(rows_of(fin, t * piece, piece), rows_of(orecv, j * piece, piece),
                  o_s.at[j], o_r.at[j], (o_devs[o - 1], mp))

    def c_ls(t):
        return pltpu.make_async_copy(rows_of(fin, t * piece, piece), rows_of(gsum, piece_at(t, zi), piece), l_s.at[t])

    def d_es(t):
        r = rows_of(gsum, t * CHUNK + y * half, half)
        return rc(r, r, e_s.at[t], e_r.at[t], dev_y)

    def d_er(t):
        r = rows_of(gsum, t * CHUNK + (1 - y) * half, half)
        return rc(r, r, e_s.at[t], e_r.at[t], dev_y)

    def get(ref, r0, n):
        return ref[pl.ds(pl.multiple_of(r0, 16), n), :].astype(F32)

    def put(ref, r0, n, val):
        ref[pl.ds(pl.multiple_of(r0, 16), n), :] = val.astype(BF16)

    def st_y(t):
        d_xs(t).wait_recv()
        r0 = t * CHUNK
        put(keep, r0, CHUNK, get(keep, r0, CHUNK) + get(xrecv, r0, CHUNK))
        d_ys(t).start()

    def st_z(t):
        d_ys(t).wait_recv()
        r0 = t * CHUNK + y * half
        put(keep, r0, half, get(keep, r0, half) + get(yrecv, t * half, half))
        for o in range(1, nz):
            d_zs(t, o).start()

    def st_a(t):
        for o in range(1, nz):
            d_zs(t, o).wait_recv()
        acc = get(keep, piece_at(t, zi), piece)
        for o in range(1, nz):
            acc = acc + get(zrecv, (t * (nz - 1) + o - 1) * piece, piece)
        put(fin, t * piece, piece, acc)
        if n_out == 1:
            st_g(t)
        else:
            for o in range(1, n_out):
                d_os(t, o).start()

    def st_o(t):
        own_part = get(fin, t * piece, piece)
        acc = own_part
        for o in range(1, n_out):
            d_os(t, o).wait_recv()
            d_os(t, o).wait_send()
        me = dp // inner
        acc = jnp.zeros_like(own_part)
        for gidx in range(n_out):
            slot = (me - gidx + n_out) % n_out
            r0 = (t * (n_out - 1) + jnp.maximum(slot, 1) - 1) * piece
            acc = acc + jnp.where(slot == 0, own_part, get(orecv, r0, piece))
        put(fin, t * piece, piece, acc)
        st_g(t)

    def st_g(t):
        c_ls(t).start()
        for o in range(1, nz):
            d_as(t, o).start()

    def st_b(t):
        c_ls(t).wait()
        for o in range(1, nz):
            d_ar(t, o).wait_recv()
        d_es(t).start()

    def st_e(t):
        d_er(t).wait_recv()
        d_xs(t).wait_send()
        d_ys(t).wait_send()
        d_es(t).wait_send()
        for o in range(1, nz):
            d_zs(t, o).wait_send()
            d_as(t, o).wait_send()

    stages = [st_y, st_z, st_a] + ([st_o] if n_out > 1 else []) + [st_b, st_e]

    gap = 2

    def tick(t):
        for s in reversed(range(len(stages))):
            u = t - gap * s

            @pl.when(jnp.logical_and(u >= 0, u < n_chunks))
            def _(s=s, u=u):
                stages[s](u)

    def d_c(slot, r0, n, j):
        part = pl.ds(pl.multiple_of(r0, 16), n)
        return rc(csend.at[slot, part, :], crecv.at[slot, part, :], c_s.at[slot, j], c_r.at[slot, j], dev_s)

    def m_of(i):
        mx = jnp.where(i < 2, 1 - x, x)
        mc = jnp.where(i % 2 == 0, 1 - c, c)
        return 2 * mx + mc

    small[...] = jnp.zeros_like(small)
    rb = 128

    def ln1(i):
        r = pl.ds(pl.multiple_of(i * rb, rb), rb)
        xv = tok[r, :].astype(F32)
        xc = xv - jnp.mean(xv, axis=-1, keepdims=True)
        inv = lax.rsqrt(jnp.mean(xc * xc, axis=-1, keepdims=True) + EPS)
        n1[r, :] = (xc * inv * g1[...] + s1[...]).astype(BF16)

    c_tok.wait()
    loop(rows // rb, ln1)

    n_seg = lens.shape[1]
    col = lax.broadcasted_iota(jnp.int32, (rows, 1), 0)
    row = lax.broadcasted_iota(jnp.int32, (1, rows), 1)
    seg_col, seg_row = jnp.zeros_like(col), jnp.zeros_like(row)
    bound = jnp.int32(0)
    for j in range(n_seg):
        bound = bound + lens[mp, j]
        seg_col = seg_col + (col >= bound).astype(jnp.int32)
        seg_row = seg_row + (row >= bound).astype(jnp.int32)
    mask[...] = jnp.where(seg_col == seg_row, 0.0, -1000000000.0).astype(F32)
    kept = (seg_col < n_seg - 1).astype(F32)

    biasg[mp] = bias[...]
    for i in range(3):
        d_bias(i).wait()
    tot = biasg[0]
    for m in range(1, 4):
        tot = tot + pltpu.roll(biasg[m], hw * m, 1)
    qvb[...] = tot

    scale = 1.0 / math.sqrt(HD)
    n_pairs = d // (2 * HD)
    per_half = n_pairs // 2
    low_half = lax.broadcasted_iota(jnp.int32, (1, 2 * HD), 1) < HD
    ab = rows // 2

    def lanes_of(i):
        xh = jnp.where(i < per_half, x, 1 - x)
        pair = xh * per_half + i % per_half
        return xh, pair, pl.ds(pl.multiple_of(pair * 2 * HD, 128), 2 * HD)

    def pick(h, val):
        zero = jnp.zeros_like(val)
        return jnp.where(low_half, val, zero) if h == 0 else jnp.where(low_half, zero, val)

    def attn_fwd(i):
        xh, pair, lanes = lanes_of(i)

        @pl.when(i == 0)
        def _():
            near(0)

        @pl.when(i == per_half)
        def _():
            far(0)
            do((1, 5))

        @pl.when(i % per_half == 0)
        def _():
            w_rows = pl.ds(pl.multiple_of(xh * half_w, 128), half_w)
            w_lanes = w_rows
            for cc, ref in enumerate((q, k, v)):
                val = nt(n1[...], wq[cc, w_rows, :])
                if cc == 0:
                    val = val + qvb[1:2, w_lanes]
                if cc == 2:
                    val = val + qvb[2:3, w_lanes]
                val = val.astype(BF16)
                if cc == 0:
                    val = val * jnp.asarray(scale, BF16)
                ref[:, w_lanes] = val

        k2, v2 = k[:, lanes], v[:, lanes]
        for r in range(2):
            rs = pl.ds(r * ab, ab)
            q2 = q[rs, lanes]
            outs = []
            for h in range(2):
                sc = nt(pick(h, q2), k2) + mask[rs, :]
                e = jnp.exp(sc - jnp.max(sc, axis=-1, keepdims=True))
                pr = (e * (1.0 / jnp.sum(e, axis=-1, keepdims=True))).astype(BF16)
                p[2 * pair + h, rs, :] = pr
                outs.append(nn(pr, v2))
            o2 = jnp.where(low_half, outs[0], outs[1]) * kept[r * ab:(r + 1) * ab]
            att[rs, lanes] = o2.astype(BF16)

            for at, todo in AG_PLAN.items():
                if at % 2 == r:
                    @pl.when(i == at // 2)
                    def _(todo=todo):
                        do(*todo)

    AG_PLAN = {
        0: [(1, 0)],
        1: [(1, 1)],
        3: [(2, 0), (1, 2)],
        5: [(2, 1), (3, 0), (2, 2), (1, 3), (3, 1), (3, 2), (1, 4)],
        6: [(2, 3), (2, 4), (3, 3)],
        7: [(1, 6), (2, 5)],
        9: [(1, 7), (3, 4)],
        10: [(3, 5)],
        11: [(1, 8), (2, 6)],
    }
    loop(n_pairs, attn_fwd)

    near(1)
    far(1)
    mixed[...] = nn(att[...], wo[...])
    do((2, 7), (3, 6))

    def ln2(i):
        r = pl.ds(pl.multiple_of(i * rb, rb), rb)
        xv = tok[r, :].astype(F32) + mixed[r, :] + ob[...]
        mixed[r, :] = xv
        lo[r, :] = xv + db[...]
        xc = xv - jnp.mean(xv, axis=-1, keepdims=True)
        inv = lax.rsqrt(jnp.mean(xc * xc, axis=-1, keepdims=True) + EPS)
        n2[r, :] = (xc * inv * g2[...] + s2[...]).astype(BF16)

    loop(rows // rb, ln2)
    do((1, 9), (2, 8), (3, 7), (1, 10))

    tile = 256

    def emit_block(g, i, make):
        slot, mine = i // 2, i % 2 == 1
        n_parts = d // tile
        if g > 0:
            @pl.when(jnp.logical_not(mine))
            def _():
                pl.semaphore_wait(credit.at[slot], 1)
                for r in range(n_parts):
                    d_c(slot, r * tile, tile, r).wait_send()

        def part(r):
            rr = pl.ds(pl.multiple_of(r * tile, tile), tile)
            res = make(r)

            @pl.when(jnp.logical_not(mine))
            def _():
                csend[slot, rr, :] = res.astype(BF16)
                d_c(slot, r * tile, tile, r).start()

            @pl.when(mine)
            def _():
                d_c(slot, r * tile, tile, r).wait_recv()
                tot = (res + crecv[slot, rr, :].astype(F32)).astype(BF16)
                out = pl.ds(pl.multiple_of(g * d + r * tile, tile), tile)

                @pl.when(slot == 0)
                def _():
                    xsend[out, :] = tot
                    for cc in range(tile // CHUNK):
                        d_xs(g * per_group + r * (tile // CHUNK) + cc).start()

                @pl.when(slot == 1)
                def _():
                    keep[out, :] = tot

        loop(n_parts, part)

        @pl.when(mine)
        def _():
            pl.semaphore_signal(credit.at[slot], inc=1, device_id=dev_s, device_id_type=MESH)

    near(2)
    far(2)

    c_cot.wait()

    def ffn1(i):
        m = m_of(i)

        def hid(n):
            nl = pl.ds(pl.multiple_of(n * tile, tile), tile)
            h = nn(n2[...], wu[m, :, nl]) + biasg[m, 0:1, nl]
            phi = 0.5 * (1.0 + lax.erf(h * INV_SQRT2))
            act[m, :, nl] = (h * phi).astype(BF16)
            gp[m, :, nl] = (phi + h * jnp.exp(-0.5 * h * h) * INV_SQRT2PI).astype(BF16)

        loop(ff // tile, hid)

        def make(r):
            rl = pl.ds(pl.multiple_of(r * tile, tile), tile)
            return tn(act[m, :, rl], cot[...])

        emit_block(0, i, make)

        for at, todo in enumerate(([(1, 11), (2, 9), (3, 8), (2, 10), (3, 9)], [(2, 11), (3, 10)], [(3, 11)])):
            @pl.when(i == at)
            def _(todo=todo):
                do(*todo)

    loop(4, ffn1)

    near(3)
    far(3)

    def c_wd(i):
        return pltpu.make_async_copy(wd_full.at[m_of(i)], wdbuf.at[i % 2], wd_sem.at[i % 2])

    def start_wd(i):
        @pl.when(i < 3)
        def _():
            c_wd(i).start()

        @pl.when(i == 3)
        def _():
            pltpu.make_async_copy(wd_in, wdbuf.at[i % 2], wd_sem.at[i % 2]).start()

    start_wd(0)
    mg[...] = jnp.zeros_like(mg)

    def ffn2(i):
        m = m_of(i)
        c_wd(i).wait()

        @pl.when(i < 3)
        def _():
            start_wd(i + 1)

        s = i % 2

        def hg(n):
            nl = pl.ds(pl.multiple_of(n * tile, tile), tile)
            val = (gp[m, :, nl].astype(F32) * nt(cot[...], wdbuf[s, nl, :])).astype(BF16)
            gp[m, :, nl] = val
            small[pl.ds(8 + m, 1), nl] = jnp.sum(val.astype(F32), axis=0, keepdims=True)

        loop(ff // tile, hg)

        def make(r):
            rl = pl.ds(pl.multiple_of(r * tile, tile), tile)
            return tn(n2[:, rl], gp[m])

        emit_block(1, i, make)
        tick(jnp.where(i < 2, 2 * i, i + 2))

        def back(n):
            nl = pl.ds(pl.multiple_of(n * tile, tile), tile)
            mg[:, nl] += nt(gp[m], wu[m, nl, :])
            lo[:, nl] += nn(act[m], wdbuf[s, :, nl])

        loop(d // tile, back)

        @pl.when(i < 2)
        def _():
            tick(2 * i + 1)

    loop(4, ffn2)
    c_lo.start()

    def ln2b(i):
        r = pl.ds(pl.multiple_of(i * rb, rb), rb)
        xv = mixed[r, :]
        xc = xv - jnp.mean(xv, axis=-1, keepdims=True)
        inv = lax.rsqrt(jnp.mean(xc * xc, axis=-1, keepdims=True) + EPS)
        xh = xc * inv
        dn = mg[r, :]
        small[2:3, :] += jnp.sum(dn * xh, axis=0, keepdims=True)
        small[3:4, :] += jnp.sum(dn, axis=0, keepdims=True)
        gg = dn * g2[...]
        val = cot[r, :].astype(F32) + (
            gg - jnp.mean(gg, axis=-1, keepdims=True) - xh * jnp.mean(gg * xh, axis=-1, keepdims=True)
        ) * inv
        mg[r, :] = val
        mgl[r, :] = val.astype(BF16)
        small[4:5, :] += jnp.sum(val, axis=0, keepdims=True)
        small[5:6, :] += jnp.sum(cot[r, :].astype(F32), axis=0, keepdims=True)

    loop(rows // rb, ln2b)

    da = n2

    def dab(n):
        nl = pl.ds(pl.multiple_of(n * tile, tile), tile)
        da[:, nl] = (nt(mgl[...], wo[nl, :]).astype(BF16).astype(F32) * kept).astype(BF16)

    loop(d // tile, dab)
    tick(6)

    def attn_bwd(i):
        xh, pair, lanes = lanes_of((i + per_half) % n_pairs)
        k2, v2 = k[:, lanes], v[:, lanes]
        do2, q2 = da[:, lanes], q[:, lanes]
        dqs, dks, dvs = [], [], []
        for h in range(2):
            dq_rows = []
            for r in range(2):
                rs = slice(r * ab, (r + 1) * ab)
                dpv = nt(pick(h, do2[rs]), v2)
                pr = p[2 * pair + h, pl.ds(r * ab, ab), :].astype(F32)
                t1 = pr * dpv
                ds = (t1 - pr * jnp.sum(t1, axis=-1, keepdims=True)).astype(BF16)
                dsb[pl.ds(r * ab, ab), :] = ds
                dq_rows.append(nn(ds, k2))
            dqs.append(jnp.concatenate(dq_rows, axis=0))
            dks.append(tn(dsb[...], q2))
            dvs.append(tn(p[2 * pair + h], do2))
        dv2 = jnp.where(low_half, dvs[0], dvs[1]).astype(BF16)
        dk2 = jnp.where(low_half, dks[0], dks[1]).astype(BF16)
        dq2 = (jnp.where(low_half, dqs[0], dqs[1]) * scale).astype(BF16)
        q[:, lanes] = dq2
        k[:, lanes] = dk2
        v[:, lanes] = dv2
        small[6:7, lanes] = jnp.sum(dq2.astype(F32), axis=0, keepdims=True)
        small[7:8, lanes] = jnp.sum(dv2.astype(F32), axis=0, keepdims=True)

        @pl.when(i % per_half == per_half - 1)
        def _():
            a = i // per_half
            wl = pl.ds(pl.multiple_of(xh * half_w, 128), half_w)
            pl.semaphore_wait(credit.at[a], 1)
            for r in range(d // tile):
                d_c(a, r * tile, tile, r).wait_send()
            for j, (ref, other) in enumerate(((att, mgl), (q, n1), (k, n1), (v, n1))):
                act[pl.ds(0, 2), pl.ds(0, hw), :] = tn(ref[:, wl], other[...]).astype(BF16).reshape(2, hw, d)
                csend[a, j * hw:(j + 1) * hw, :] = act[1 - c, 0:hw, :]
                d_c(a, j * hw, hw, j).start()
                gp[0 if j < 2 else 1, (j % 2) * hw:(j % 2 + 1) * hw, :] = act[c, 0:hw, :]
            for j in range(4):
                d_c(a, j * hw, hw, j).wait_recv()
                tot = (gp[0 if j < 2 else 1, (j % 2) * hw:(j % 2 + 1) * hw, :].astype(F32)
                       + crecv[a, j * hw:(j + 1) * hw, :].astype(F32)).astype(BF16)

                @pl.when(a == 0)
                def _():
                    xsend[2 * d + j * hw:2 * d + (j + 1) * hw, :] = tot

                @pl.when(a == 1)
                def _():
                    keep[2 * d + j * hw:2 * d + (j + 1) * hw, :] = tot

            @pl.when(a == 0)
            def _():
                for cc in range(per_group):
                    d_xs(2 * per_group + cc).start()

        tick(7 + i)

    loop(n_pairs, attn_bwd)

    def ln1n(n):
        nl = pl.ds(pl.multiple_of(n * tile, tile), tile)
        tg[:, nl] = nn(q[...], wq[0, :, nl]) + nn(k[...], wq[1, :, nl]) + nn(v[...], wq[2, :, nl])

    loop(d // tile, ln1n)

    def ln1b(i):
        r = pl.ds(pl.multiple_of(i * rb, rb), rb)
        xv = tok[r, :].astype(F32)
        xc = xv - jnp.mean(xv, axis=-1, keepdims=True)
        inv = lax.rsqrt(jnp.mean(xc * xc, axis=-1, keepdims=True) + EPS)
        xh = xc * inv
        dn = tg[r, :]
        small[0:1, :] += jnp.sum(dn * xh, axis=0, keepdims=True)
        small[1:2, :] += jnp.sum(dn, axis=0, keepdims=True)
        gg = dn * g1[...]
        tg[r, :] = mg[r, :] + (
            gg - jnp.mean(gg, axis=-1, keepdims=True) - xh * jnp.mean(gg * xh, axis=-1, keepdims=True)
        ) * inv

    loop(rows // rb, ln1b)
    c_tg.start()

    v_devs = [(dp, sib), (dp, xn)] + [(flip(dp, b), mp) for b in bits]

    def d_v(s):
        return rc(small, srecv.at[s], v_s.at[s], v_r.at[s], v_devs[s])

    first = 7 + n_pairs

    def tail(i):
        for s in range(len(v_devs) + 1):
            @pl.when(i == s)
            def _(s=s):
                if s > 0:
                    d_v(s - 1).wait()
                    small[...] += srecv[s - 1]
                if s < len(v_devs):
                    d_v(s).start()

        tick(first + i)

    loop(max(n_chunks + gap * (len(stages) - 1) - first, len(v_devs) + 1), tail)
    for slot in range(2):
        for j in range(4):
            d_c(slot, j * hw, hw, j).wait_send()
    sent()
    c_lo.wait()
    c_tg.wait()


def layer(n_dp, tokens, lens, g1, s1, wqkv, qvb, wo, ob, g2, s2, wu, ub, wd, db, cot):
    rows, d = tokens.shape
    hw, ff = wo.shape[0], wu.shape[1]
    n_mp = lax.axis_size("mp")
    mp = lax.axis_index("mp")
    inner = min(n_dp, 8)
    nz, n_out = inner // 2, n_dp // inner
    piece = CHUNK // 2 // nz
    nc = 3 * d // CHUNK
    n_small = 2 + n_dp.bit_length() - 1
    heads = d // HD
    wqt = jnp.swapaxes(wqkv, 1, 2)
    vm = pl.BlockSpec(memory_space=pltpu.VMEM)
    hbm = pl.BlockSpec(memory_space=pl.ANY)
    sm = pl.BlockSpec(memory_space=pltpu.SMEM)
    dma = pltpu.SemaphoreType.DMA
    S = jax.ShapeDtypeStruct
    V = pltpu.VMEM
    nzr = max(nc * (nz - 1), 1)
    nor = max(nc * (n_out - 1), 1)
    lo, tg, gsum, small, _ = pl.pallas_call(
        functools.partial(body, n_dp),
        out_shape=(
            S((rows, d), F32), S((rows, d), F32), S((3 * d, d), BF16), S((16, d), F32), S((n_mp, ff, d), BF16),
        ),
        in_specs=[sm] + [hbm] * 2 + [vm] * 8 + [hbm] * 4,
        out_specs=(hbm, hbm, hbm, vm, hbm),
        scratch_shapes=[
            V((rows, d), BF16), V((rows, d), BF16), V((rows, d), F32), V((rows, d), F32), V((8, d), F32), V((8, d), F32),
            V((8, d), F32),
            V((3, d, d), BF16), V((d, d), BF16), V((n_mp, d, ff), BF16), V((2, ff, d), BF16), V((n_mp, 8, d), F32),
            V((rows, d), BF16), V((rows, d), BF16), V((rows, d), BF16), V((rows, d), BF16),
            V((heads, rows, rows), BF16), V((rows, rows), BF16), V((rows, d), BF16),
            V((rows, d), F32), V((rows, d), F32), V((rows, d), BF16), V((rows, d), BF16),
            V((n_mp, rows, ff), BF16), V((n_mp, rows, ff), BF16), V((rows, rows), F32),
            V((2, d, d), BF16), V((2, d, d), BF16), V((3 * d, d), BF16), V((3 * d, d), BF16), V((3 * d, d), BF16),
            V((nc * CHUNK // 2, d), BF16), V((nzr * piece, d), BF16), V((nc * piece, d), BF16),
            V((nor * piece, d), BF16), V((n_small, 16, d), F32),
            dma((4,)), dma((4,)), dma((4,)), dma((4,)), dma((4,)), dma((12, 8)), dma((12, 4)), dma((3,)), dma((3,)),
            dma((2,)), dma((2, 4)), dma((2, 4)),
            pltpu.SemaphoreType.REGULAR((2,)), dma((nc,)), dma((nc,)), dma((nc,)), dma((nc,)),
            dma((nzr,)), dma((nzr,)), dma((nzr,)), dma((nzr,)), dma((nc,)), dma((nc,)), dma((nc,)),
            dma((nor,)), dma((nor,)), dma((n_small,)), dma((n_small,)),
        ],
        compiler_params=pltpu.CompilerParams(
            collective_id=0, has_side_effects=True, vmem_limit_bytes=67043328
        ),
        name="layer",
    )(lens, tokens, cot, g1, s1, ob, g2, s2, db, ub, qvb, wqt, wo, wu, wd)

    steps = 4
    part, rpart = d // steps, rows // steps
    opart = hw

    def finish(down, up, rest, lo_ref, tg_ref, sm_ref, o_down, o_up, o_out, o_qkv, o_lo, o_tg,
               o_g1, o_s1, o_g2, o_s2, o_ob, o_db, o_qv, o_ub):
        i = pl.program_id(0)
        o_down[...] = down[...].astype(F32)
        o_up[...] = up[...].astype(F32)
        o_lo[...] = lo_ref[...]
        o_tg[...] = tg_ref[...]

        @pl.when(i == 0)
        def _():
            o_out[...] = rest[...].astype(F32)

        @pl.when(i > 0)
        def _():
            o_qkv[0] = rest[...].astype(F32)

        @pl.when(i == 0)
        def _():
            for n, ref in enumerate((o_g1, o_s1, o_g2, o_s2, o_ob, o_db)):
                ref[...] = sm_ref[n:n + 1, :].reshape(d)
            me = lax.axis_index("mp")
            o_ub[...] = sm_ref[pl.ds(8 + me, 1), :].reshape(d)
            acc = jnp.zeros((2, hw), F32)
            for m in range(n_mp):
                acc = jnp.where(me == m, sm_ref[6:8, m * hw:(m + 1) * hw], acc)
            o_qv[...] = acc

    blk = lambda off: pl.BlockSpec((part, d), lambda i: (i + off, 0))
    row = pl.BlockSpec((rpart, d), lambda i: (i, 0))
    one = pl.BlockSpec((d,), lambda i: (0,))
    dwn, up_g, out_g, qkv_g, lo, tg, o_g1, o_s1, o_g2, o_s2, o_ob, o_db, o_qv, o_ub = pl.pallas_call(
        finish,
        grid=(steps,),
        out_shape=(
            S((ff, d), F32), S((d, ff), F32), S((hw, d), F32), S((3, hw, d), F32), S((rows, d), F32), S((rows, d), F32),
            S((d,), F32), S((d,), F32), S((d,), F32), S((d,), F32), S((d,), F32), S((d,), F32), S((2, hw), F32), S((d,), F32),
        ),
        in_specs=[blk(0), blk(steps), blk(2 * steps), row, row, pl.BlockSpec((16, d), lambda i: (0, 0))],
        out_specs=(
            blk(0), blk(0), pl.BlockSpec((opart, d), lambda i: (0, 0)),
            pl.BlockSpec((1, opart, d), lambda i: (jnp.maximum(i - 1, 0), 0, 0)), row, row,
            one, one, one, one, one, one, pl.BlockSpec((2, hw), lambda i: (0, 0)), one,
        ),
        name="finish",
    )(gsum, gsum, gsum, lo, tg, small)
    return (
        lo, tg, o_g1, o_s1, jnp.swapaxes(qkv_g, 1, 2), o_qv, out_g, o_ob, o_g2, o_s2, up_g, o_ub, dwn, o_db,
    )


def solution(mesh):
    rows = P(("dp", "mp"), None)
    in_specs = (
        rows, P("dp", None), P(), P(), P(None, None, "mp"), P(None, "mp"), P("mp", None), P(), P(), P(),
        P(None, "mp"), P("mp"), P("mp", None), P(), rows,
    )
    out_specs = (
        rows, rows, P(), P(), P(None, None, "mp"), P(None, "mp"), P("mp", None), P(), P(), P(),
        P(None, "mp"), P("mp"), P("mp", None), P(),
    )
    return jax.shard_map(
        functools.partial(layer, mesh.shape["dp"]), mesh=mesh, in_specs=in_specs, out_specs=out_specs, check_vma=False
    )
```
